256 devices in a mesh: gz: 32 (over x, y, core), xy: 8 (over z).
Axes of the slice: x: 4, y: 4, z: 8, core: 2. Of those that a mesh axis runs over, the one named last changes fastest.
Arguments:
- east_velocity: float32 [512, 256, 512], P('xy', 'gz'), may hold values from -6 to 6
- north_velocity: float32 [512, 256, 512], P('xy', 'gz'), may hold values from -6 to 6
- upward_velocity: float32 [512, 256, 512], P('xy', 'gz'), may hold values from -5 to 5
- obstacle: int32 [512, 256, 512], P('xy', 'gz'), may hold values 0 or 1
Outputs:
- east_corrected: float32 [512, 256, 512], P('xy', 'gz')
- north_corrected: float32 [512, 256, 512], P('xy', 'gz')
- upward_corrected: float32 [512, 256, 512], P('xy', 'gz')
- pressure: float32 [512, 256, 512], P('xy', 'gz')
- residual: float32 [512, 256, 512], P('xy', 'gz')
The draws below stay inside these ranges and needn't reach their ends.
All inputs are finite; a program needn't handle non-finite values. No bound on the sum of `obstacle` on one device may be relied on, other than what follows from the above.
Results may differ from the reference program's by a relative error of at most 0.0003.
Values sent between devices are 32-bit elements; how exact they have to be, the bound alone decides.
A program may use at most 128 MiB of HBM per device.

```python
import jax
import jax.numpy as jnp
from jax import lax

NX = 512
NY = 512
NZ = 256


def draw_upward_velocity(key, part):
    base = jnp.clip(jax.random.normal(jax.random.fold_in(key, 17), (NX, NZ, NY), jnp.float32), -5.0, 5.0)
    return base


def plant(drawn, own_key, smallest, top_value):
    dims = drawn.shape
    spot = [jax.random.randint(jax.random.fold_in(own_key, axis), (), 0, dims[axis]) for axis in range(len(dims))]
    drawn = drawn.at[tuple(spot)].set(smallest)
    longest = dims.index(max(dims))
    spot[longest] = (spot[longest] + 1) % dims[longest]
    return drawn.at[tuple(spot)].set(top_value)


def block_scale(rng, shape, split, least, high):
    def one(dim, blocks):
        draws = jax.random.uniform(jax.random.fold_in(jax.random.fold_in(rng, 6), dim), (blocks,), jnp.float32, least / len(split), high / len(split))
        return jnp.repeat(jnp.exp(draws), shape[dim] // blocks).reshape((-1,) + (1,) * (len(shape) - dim - 1))

    level = one(*split[0])
    for cut in split[1:]:
        level = level * one(*cut)
    return level


def noise(key, dims, width, reach, pieces=(), kind=jnp.bfloat16):
    values = width * jax.random.normal(key, dims, jnp.float32)
    if pieces:
        values = values * block_scale(key, dims, pieces, -0.22, 0.18)
    return jnp.clip(values, -reach, reach).astype(kind)


def setup_inputs(seed: int = 0) -> dict:
    key_list = jax.random.split(jax.random.key(seed), 5)
    return {
        "east_velocity": noise(key_list[0], (NX, NZ, NY), 1.0, 6.0, ((0, 8), (1, 32)), jnp.float32),
        "north_velocity": noise(key_list[1], (NX, NZ, NY), 1.0, 6.0, ((0, 8), (1, 32)), jnp.float32),
        "upward_velocity": draw_upward_velocity(jax.random.fold_in(key_list[4], 71), 0),
        "obstacle": plant((jax.random.randint(key_list[3], (NX, NZ, NY), 0, 6) < 1).astype(jnp.int32), jax.random.fold_in(key_list[3], 1), 0, 1),
    }


HIGH = lax.Precision.HIGHEST


def hartley(length):
    index = jnp.arange(length, dtype=jnp.int32)
    product = (index[:, None] * index[None, :]) % length
    angle = (2.0 * jnp.pi / length) * product.astype(jnp.float32)
    return jnp.cos(angle) + jnp.sin(angle)


def eigenvalues(length):
    index = jnp.arange(length, dtype=jnp.int32).astype(jnp.float32)
    return 2.0 - 2.0 * jnp.cos((2.0 * jnp.pi / length) * index)


def tridiagonal(diagonal, right):
    start = jnp.zeros_like(right[0])

    def forward(carry, plane):
        ratio, value = carry
        divisor = diagonal + ratio
        ratio_new = -1.0 / divisor
        value_new = (plane + value) / divisor
        return (ratio_new, value_new), (ratio_new, value_new)

    _, (ratios, values) = lax.scan(forward, (start, start), right)

    def backward(after, pair):
        ratio, value = pair
        solution = value - ratio * after
        return solution, solution

    _, solved = lax.scan(backward, start, (ratios, values), reverse=True)
    return solved


def reference(east_velocity, north_velocity, upward_velocity, obstacle):
    fluid = (1 - obstacle).astype(jnp.float32)
    ones_plane = jnp.ones((NX, 1, NY), jnp.float32)
    zero_plane = jnp.zeros((NX, 1, NY), jnp.float32)
    open_east = fluid * jnp.roll(fluid, 1, 0)
    open_north = fluid * jnp.roll(fluid, 1, 2)
    open_up = fluid * jnp.concatenate([ones_plane, fluid[:, :-1]], 1)
    east_masked = open_east * east_velocity
    north_masked = open_north * north_velocity
    upward_masked = open_up * upward_velocity
    east_after = jnp.roll(east_masked, -1, 0)
    upward_after = jnp.concatenate([upward_masked[:, 1:], zero_plane], 1)
    source = (east_masked - east_after) + (north_masked - jnp.roll(north_masked, -1, 2)) + (upward_masked - upward_after)
    table_east = hartley(NX)
    table_north = hartley(NY)
    partial_modes = jnp.einsum("xzy,ky->xzk", source, table_north, precision=HIGH)
    spectrum = jnp.einsum("xzk,xa->zka", partial_modes, table_east, precision=HIGH)
    diagonal = 2.0 + eigenvalues(NY)[:, None] + eigenvalues(NX)[None, :]
    modes = tridiagonal(diagonal, spectrum)
    half_back = jnp.einsum("zka,xa->xzk", modes, table_east, precision=HIGH)
    pressure = jnp.einsum("xzk,yk->xzy", half_back, table_north, precision=HIGH) * (1.0 / (NX * NY))
    west_full = jnp.roll(pressure, 1, 0)
    east_full = jnp.roll(pressure, -1, 0)
    below_full = jnp.concatenate([zero_plane, pressure[:, :-1]], 1)
    above_full = jnp.concatenate([pressure[:, 1:], zero_plane], 1)
    open_east_after = jnp.roll(open_east, -1, 0)
    open_north_after = jnp.roll(open_north, -1, 2)
    open_up_after = jnp.concatenate([open_up[:, 1:], zero_plane], 1)
    applied = (open_east * (pressure - west_full) + open_east_after * (pressure - east_full)
               + open_north * (pressure - jnp.roll(pressure, 1, 2)) + open_north_after * (pressure - jnp.roll(pressure, -1, 2))
               + open_up * (pressure - below_full) + open_up_after * (pressure - above_full))
    residual = source - applied
    east_corrected = open_east * (east_velocity - (pressure - west_full))
    north_corrected = open_north * (north_velocity - (pressure - jnp.roll(pressure, 1, 2)))
    upward_corrected = open_up * (upward_velocity - (pressure - below_full))
    return east_corrected, north_corrected, upward_corrected, pressure, residual
```

```python
import functools

import jax
import jax.numpy as jnp
import numpy as np
from jax import lax
from jax.experimental import pallas as pl
from jax.experimental.pallas import tpu as pltpu
from jax.sharding import PartitionSpec as P

NX = 512
NY = 512
NZ = 256
GZ = 32
XY = 8
XR = NX // XY
CZ = NZ // GZ
NH = 2
KL = NY // GZ // NH
XL = 128 // KL
J = XR // XL
LH = NY // NH
W = J * 128
ROWS = XR * CZ
F32 = jnp.float32
BF16 = jnp.bfloat16


def split(a):
    hi = a.astype(BF16)
    return hi, (a - hi.astype(F32)).astype(BF16)


def dot(a, b):
    return jnp.dot(a, b, preferred_element_type=F32)


def dot3(a, b):
    return dot(a[0], b[0]) + (dot(a[0], b[1]) + dot(a[1], b[0]))


def lanes(shape):
    return lax.broadcasted_iota(jnp.int32, shape, 1)


def roll(a, shift):
    return pltpu.roll(a, shift % 128, 1)


def exchange_lanes(tiles):
    tiles = list(tiles)
    group = lanes((8, 128)) // KL
    step = 1
    while step < XL:
        clear = (group & step) == 0
        for i in range(XL):
            if not i & step:
                k = i | step
                a, b = tiles[i], tiles[k]
                tiles[i] = jnp.where(clear, a, roll(b, step * KL))
                tiles[k] = jnp.where(clear, roll(a, -step * KL), b)
        step *= 2
    return tiles


def main_kernel(
    e_h, n_h, w_h, o_h, hh_h, hl_h, sh_h, sl_h, lam_h, mu_h, mup_h,
    p_v, f_v, src_v, zp_v, zf_v,
    e_v, n_v, w_v, o_v, hh, hl, sh, sl, lam, mu, mup,
    wa_v, zs_v, zps_v, y_v, send1, recv1, dh, dl, x_v, ea_v, eb_v, r_v, c_v, ag_v, uv_v, send2, recv2, zz_v,
    load_sem, halo_s, halo_r, a_s, a_r, g_s, g_r, b_s, b_r, ph_s, ph_r,
):
    me = lax.axis_index("gz")
    xi = lax.axis_index("xy")

    def gz(o):
        return {"gz": lax.rem(me + o, GZ)}

    def xy(o):
        return {"xy": lax.rem(xi + o, XY)}

    def load(k, src, dst):
        copy = pltpu.make_async_copy(src, dst, load_sem.at[k])
        copy.start()
        return copy

    def remote(src, dst, ssem, rsem, who):
        copy = pltpu.make_async_remote_copy(
            src_ref=src, dst_ref=dst, send_sem=ssem, recv_sem=rsem, device_id=who,
            device_id_type=pl.DeviceIdType.MESH,
        )
        copy.start()
        return copy

    loads = [
        load(0, o_h, o_v),
        load(1, w_h, w_v),
        load(2, e_h, e_v.at[pl.ds(0, ROWS)]),
        load(3, n_h, n_v),
        load(4, hh_h, hh),
        load(5, hl_h, hl),
        load(6, sh_h, sh),
        load(7, sl_h, sl),
        load(8, lam_h, lam),
        load(9, mu_h, mu),
        load(10, mup_h, mup),
    ]

    barrier = pltpu.get_barrier_semaphore()

    def greet_gz(o, _):
        pl.semaphore_signal(barrier, inc=1, device_id=gz(o), device_id_type=pl.DeviceIdType.MESH)
        return 0

    def greet_xy(o, _):
        pl.semaphore_signal(barrier, inc=1, device_id=xy(o), device_id_type=pl.DeviceIdType.MESH)
        return 0

    lax.fori_loop(1, GZ, greet_gz, 0)
    lax.fori_loop(1, XY, greet_xy, 0)

    loads[0].wait()

    def to_fluid(i, _):
        rows = pl.ds(pl.multiple_of(i * 64, 64), 64)
        f_v[pl.ds(pl.multiple_of(8 + i * 64, 8), 64), :] = (1 - o_v[rows, :]).astype(F32)
        return 0

    lax.fori_loop(0, ROWS // 64, to_fluid, 0)
    loads[1].wait()
    loads[2].wait()

    def edge(i, _):
        for k in range(8):
            x = i * 8 + k
            zs_v[pl.ds(x, 1), :] = f_v[pl.ds(x * 8 + 15, 1), :]
            zs_v[pl.ds(XR + x, 1), :] = f_v[pl.ds(x * 8 + 8, 1), :]
            zs_v[pl.ds(2 * XR + x, 1), :] = w_v[pl.ds(x * 8, 1), :]
        return 0

    lax.fori_loop(0, XR // 8, edge, 0)
    pl.semaphore_wait(barrier, GZ - 1 + XY - 1)
    halos = [
        remote(zs_v.at[pl.ds(2 * XR, XR)], wa_v, halo_s.at[0], halo_r.at[0], gz(GZ - 1)),
        remote(zs_v.at[pl.ds(XR, XR)], zf_v.at[pl.ds(XR, XR)], halo_s.at[1], halo_r.at[1], gz(GZ - 1)),
        remote(zs_v.at[pl.ds(0, XR)], zf_v.at[pl.ds(0, XR)], halo_s.at[2], halo_r.at[2], gz(1)),
        remote(f_v.at[pl.ds(ROWS, 8)], f_v.at[pl.ds(0, 8)], halo_s.at[3], halo_r.at[3], xy(1)),
        remote(f_v.at[pl.ds(8, 8)], f_v.at[pl.ds(ROWS + 8, 8)], halo_s.at[4], halo_r.at[4], xy(XY - 1)),
        remote(e_v.at[pl.ds(0, 8)], e_v.at[pl.ds(ROWS, 8)], halo_s.at[5], halo_r.at[5], xy(XY - 1)),
    ]
    loads[3].wait()
    for k in range(4, 11):
        loads[k].wait()
    for h in halos:
        h.wait()

    sub = lax.broadcasted_iota(jnp.int32, (8, NY), 0)
    first = me == 0
    last = me == GZ - 1

    def source(i, _):
        base = pl.multiple_of(i * 8, 8)
        here = pl.ds(base, 8)
        f = f_v[pl.ds(pl.multiple_of(base + 8, 8), 8), :]
        fw = f_v[here, :]
        fe = f_v[pl.ds(pl.multiple_of(base + 16, 8), 8), :]
        east = f * (fw * e_v[here, :] - fe * e_v[pl.ds(pl.multiple_of(base + 8, 8), 8), :])
        fn = f * pltpu.roll(f, 1, 1) * n_v[here, :]
        north = fn - pltpu.roll(fn, NY - 1, 1)
        w = w_v[here, :]
        below = jnp.broadcast_to(zf_v[pl.ds(i, 1), :], (8, NY))
        above = jnp.broadcast_to(zf_v[pl.ds(XR + i, 1), :], (8, NY))
        wabove = jnp.broadcast_to(wa_v[pl.ds(i, 1), :], (8, NY))
        below = jnp.where(first, 1.0, below)
        above = jnp.where(last, 0.0, above)
        fb = jnp.where(sub == 0, below, pltpu.roll(f, 1, 0))
        fa = jnp.where(sub == 7, above, pltpu.roll(f, 7, 0))
        wn = jnp.where(sub == 7, wabove, pltpu.roll(w, 7, 0))
        up = f * (fb * w - fa * wn)
        src_v[here, :] = east + north + up
        return 0

    lax.fori_loop(0, XR, source, 0)

    def wait_bytes(ref, sem):
        pltpu.make_async_copy(ref, ref, sem).wait()

    for h in range(NH):
        hcol = pl.ds(h * LH, LH)

        def forward(i, _):
            rows = pl.ds(pl.multiple_of(i * 256, 256), 256)
            y_v[rows, :] = dot3(split(src_v[rows, :]), (hh[:, hcol], hl[:, hcol]))
            return 0

        lax.fori_loop(0, ROWS // 256, forward, 0)

        def pack(j, _):
            for t in range(LH // 128):
                tiles = exchange_lanes(
                    [y_v[pl.ds(pl.multiple_of((x * J + j) * 8, 8), 8), pl.ds(t * 128, 128)] for x in range(XL)]
                )
                for a in range(XL):
                    send1[pl.ds((h * GZ + t * XL + a) * 8, 8), pl.ds(pl.multiple_of(j * 128, 128), 128)] = tiles[a]
            return 0

        lax.fori_loop(0, J, pack, 0)

        mine = pl.ds(pl.multiple_of(h * NZ + me * 8, 8), 8)

        def go(o, _):
            to = lax.rem(me + o, GZ)
            remote(
                send1.at[pl.ds(pl.multiple_of((h * GZ + to) * 8, 8), 8)], recv1.at[mine],
                a_s.at[h], a_r.at[h], {"gz": to},
            )
            return 0

        lax.fori_loop(1, GZ, go, 0)
        recv1[mine, :] = send1[pl.ds(pl.multiple_of((h * GZ + me) * 8, 8), 8), :]

    for h in range(NH):
        lrow = lam[pl.ds(h * GZ + me, 1), :]

        def rates(i, _):
            rows = pl.ds(pl.multiple_of(i * 16, 16), 16)
            out = pl.ds(pl.multiple_of(h * NZ + i * 16, 16), 16)
            g = mu[rows, :] + lrow
            root = jnp.sqrt(g + 0.25 * g * g)
            r_v[out, :] = 1.0 / (1.0 + 0.5 * g + root)
            c_v[out, :] = (1.0 / (NZ + 1) / NY) / root
            return 0

        lax.fori_loop(0, NZ // 16, rates, 0)

    group = lanes((16, 128)) // KL

    def squares(r):
        out = [r]
        for _ in range(5):
            out.append(out[-1] * out[-1])
        return out

    LOGJ = J.bit_length() - 1
    LOGX = XL.bit_length() - 1

    for h in range(NH):
        wait_bytes(recv1.at[pl.ds(h * NZ, NZ - 8)], a_r.at[h])

        def cut(i, _):
            rows = pl.ds(pl.multiple_of(i * 16, 16), 16)
            a, b = split(recv1[pl.ds(pl.multiple_of(h * NZ + i * 16, 16), 16), :])
            dh[rows, :] = a
            dl[rows, :] = b
            return 0

        lax.fori_loop(0, NZ // 16, cut, 0)
        for c in range(W // 256):
            col = pl.ds(c * 256, 256)
            x_v[pl.ds(h * NZ, NZ), col] = dot3((sh[...], sl[...]), (dh[:, col], dl[:, col]))

        def sums(q, carry):
            pa, pb = carry
            rows = pl.ds(pl.multiple_of(h * NZ + q * 16, 16), 16)
            r = r_v[rows, :]
            s = [x_v[rows, pl.ds(j * 128, 128)] for j in range(J)]
            u = [s[0]]
            for j in range(1, J):
                u.append(s[j] + r * u[-1])
            v = [s[-1]]
            for j in range(J - 2, -1, -1):
                v.append(s[j] + r * v[-1])
            v = v[::-1]
            for j in range(J):
                x_v[rows, pl.ds(j * 128, 128)] = u[j] + v[j] - s[j]
            a, b = u[-1], v[0]
            pw = r
            for _ in range(LOGJ):
                pw = pw * pw
            step = 1
            while step < XL:
                a = a + jnp.where(group >= step, pw * roll(a, step * KL), 0.0)
                b = b + jnp.where(group < XL - step, pw * roll(b, -step * KL), 0.0)
                pw = pw * pw
                step *= 2
            ea_v[rows, :] = jnp.where(group >= 1, roll(a, KL), 0.0)
            eb_v[rows, :] = jnp.where(group < XL - 1, roll(b, -KL), 0.0)
            at = group == q
            pa = jnp.where(at, pltpu.roll(a, lax.rem((q + 1) * KL, 128), 1), pa)
            pb = jnp.where(at, pltpu.roll(b, q * KL, 1), pb)
            return pa, pb

        zero = jnp.zeros((16, 128), F32)
        pa, pb = lax.fori_loop(0, NZ // 16, sums, (zero, zero))
        own = pl.ds(pl.multiple_of((h * XY + xi) * 32, 32), 32)
        ag_v[pl.ds(pl.multiple_of((h * XY + xi) * 32, 32), 16), :] = pa
        ag_v[pl.ds(pl.multiple_of((h * XY + xi) * 32 + 16, 16), 16), :] = pb

        def spread(o, _):
            remote(ag_v.at[own], ag_v.at[own], g_s.at[h], g_r.at[h], xy(o))
            return 0

        lax.fori_loop(1, XY, spread, 0)

    for h in range(NH):
        wait_bytes(ag_v.at[pl.ds(h * XY * 32, (XY - 1) * 32)], g_r.at[h])
        g = mup[...] + lam[pl.ds(h * GZ + me, 1), :]
        rp = 1.0 / (1.0 + 0.5 * g + jnp.sqrt(g + 0.25 * g * g))
        for _ in range(XR.bit_length() - 1):
            rp = rp * rp
        full = rp
        for _ in range(XY.bit_length() - 1):
            full = full * full
        close = 1.0 / (1.0 - full)

        def piece(o, part):
            at = (h * XY + lax.rem(xi + o, XY)) * 32 + part * 16
            return ag_v[pl.ds(pl.multiple_of(at, 16), 16), :]

        un, vn = piece(0, 0), piece(0, 1)
        for o in range(1, XY):
            un = un * rp + piece(o, 0)
            vn = vn * rp + piece(XY - o, 1)
        un = un * close
        vn = vn * close

        def finish(q, _):
            rows = pl.ds(pl.multiple_of(h * NZ + q * 16, 16), 16)
            out = pl.ds(pl.multiple_of(q * 16, 16), 16)
            at = group == q
            ub = jnp.where(at, un, 0.0)
            vb = jnp.where(at, vn, 0.0)
            step = 1
            while step < XL:
                ub = ub + roll(ub, step * KL)
                vb = vb + roll(vb, step * KL)
                step *= 2
            r = r_v[rows, :]
            powers = [r]
            for _ in range(J - 1):
                powers.append(powers[-1] * r)
            pw = powers[-1]
            up = jnp.ones_like(r)
            down = jnp.ones_like(r)
            step = 1
            while step < XL:
                on = (group & step) != 0
                up = jnp.where(on, up * pw, up)
                down = jnp.where(on, down, down * pw)
                pw = pw * pw
                step *= 2
            cu = ea_v[rows, :] + up * ub
            cv = eb_v[rows, :] + down * vb
            c = c_v[rows, :]
            for j in range(J):
                col = pl.ds(j * 128, 128)
                sol = c * (x_v[rows, col] + powers[j] * cu + powers[J - 1 - j] * cv)
                a, b = split(sol)
                dh[out, col] = a
                dl[out, col] = b
            return 0

        lax.fori_loop(0, NZ // 16, finish, 0)
        for c in range(W // 256):
            col = pl.ds(c * 256, 256)
            send2[pl.ds(h * NZ, NZ), col] = dot3((sh[...], sl[...]), (dh[:, col], dl[:, col]))

        mine = pl.ds(pl.multiple_of((h * GZ + me) * 8, 8), 8)

        def back(o, _):
            to = lax.rem(me + o, GZ)
            remote(
                send2.at[pl.ds(pl.multiple_of(h * NZ + to * 8, 8), 8)], recv2.at[mine],
                b_s.at[h], b_r.at[h], {"gz": to},
            )
            return 0

        lax.fori_loop(1, GZ, back, 0)
        recv2[mine, :] = send2[pl.ds(pl.multiple_of(h * NZ + me * 8, 8), 8), :]

    for h in range(NH):
        wait_bytes(recv2.at[pl.ds(h * NZ, NZ - 8)], b_r.at[h])

        def unpack(j, _):
            for t in range(LH // 128):
                tiles = exchange_lanes(
                    [
                        recv2[pl.ds((h * GZ + t * XL + a) * 8, 8), pl.ds(pl.multiple_of(j * 128, 128), 128)]
                        for a in range(XL)
                    ]
                )
                for x in range(XL):
                    zz_v[pl.ds(pl.multiple_of((x * J + j) * 8, 8), 8), pl.ds(t * 128, 128)] = tiles[x]
            return 0

        lax.fori_loop(0, J, unpack, 0)

        def inverse(i, _):
            rows = pl.ds(pl.multiple_of(i * 256, 256), 256)
            out = pl.ds(pl.multiple_of(8 + i * 256, 8), 256)
            hrow = pl.ds(h * LH, LH)
            part = dot3(split(zz_v[rows, :]), (hh[hrow, :], hl[hrow, :]))
            p_v[out, :] = part if h == 0 else p_v[out, :] + part
            return 0

        lax.fori_loop(0, ROWS // 256, inverse, 0)

    def pedge(i, _):
        for k in range(8):
            x = i * 8 + k
            zps_v[pl.ds(x, 1), :] = p_v[pl.ds(x * 8 + 15, 1), :]
            zps_v[pl.ds(XR + x, 1), :] = p_v[pl.ds(x * 8 + 8, 1), :]
        return 0

    lax.fori_loop(0, XR // 8, pedge, 0)
    planes = [
        remote(zps_v.at[pl.ds(0, XR)], zp_v.at[pl.ds(0, XR)], ph_s.at[0], ph_r.at[0], gz(1)),
        remote(zps_v.at[pl.ds(XR, XR)], zp_v.at[pl.ds(XR, XR)], ph_s.at[1], ph_r.at[1], gz(GZ - 1)),
        remote(p_v.at[pl.ds(ROWS, 8)], p_v.at[pl.ds(0, 8)], ph_s.at[2], ph_r.at[2], xy(1)),
        remote(p_v.at[pl.ds(8, 8)], p_v.at[pl.ds(ROWS + 8, 8)], ph_s.at[3], ph_r.at[3], xy(XY - 1)),
    ]
    for h in range(NH):
        wait_bytes(send1.at[pl.ds(h * NZ, NZ - 8)], a_s.at[h])
        wait_bytes(ag_v.at[pl.ds(h * XY * 32, (XY - 1) * 32)], g_s.at[h])
        wait_bytes(send2.at[pl.ds(h * NZ, NZ - 8)], b_s.at[h])
    for c in planes:
        c.wait()


def last_kernel(e, n, w, src, p_v, f_v, zp, zf, eo, no, wo, po, ro):
    step = pl.program_id(0)
    me = lax.axis_index("gz")
    first = me == 0
    last = me == GZ - 1
    sub = lax.broadcasted_iota(jnp.int32, (8, NY), 0)

    def one(i, _):
        here = pl.ds(pl.multiple_of(i * 8, 8), 8)
        x = step * 8 + i
        base = pl.multiple_of(x * 8, 8)
        mid = pl.ds(pl.multiple_of(base + 8, 8), 8)
        east = pl.ds(pl.multiple_of(base + 16, 8), 8)
        p = p_v[mid, :]
        f = f_v[mid, :]
        below = jnp.where(first, 1.0, jnp.broadcast_to(zf[pl.ds(x, 1), :], (8, NY)))
        above = jnp.where(last, 0.0, jnp.broadcast_to(zf[pl.ds(XR + x, 1), :], (8, NY)))
        pbelow = jnp.where(first, 0.0, jnp.broadcast_to(zp[pl.ds(x, 1), :], (8, NY)))
        pabove = jnp.broadcast_to(zp[pl.ds(XR + x, 1), :], (8, NY))
        oe = f * f_v[pl.ds(base, 8), :]
        oe_next = f * f_v[east, :]
        on = f * pltpu.roll(f, 1, 1)
        on_next = pltpu.roll(on, NY - 1, 1)
        ou = f * jnp.where(sub == 0, below, pltpu.roll(f, 1, 0))
        ou_next = f * jnp.where(sub == 7, above, pltpu.roll(f, 7, 0))
        de = p - p_v[pl.ds(base, 8), :]
        de_next = p - p_v[east, :]
        dn = p - pltpu.roll(p, 1, 1)
        dn_next = p - pltpu.roll(p, NY - 1, 1)
        du = p - jnp.where(sub == 0, pbelow, pltpu.roll(p, 1, 0))
        du_next = p - jnp.where(sub == 7, pabove, pltpu.roll(p, 7, 0))
        applied = oe * de + oe_next * de_next + on * dn + on_next * dn_next + ou * du + ou_next * du_next
        ro[here, :] = src[here, :] - applied
        eo[here, :] = oe * (e[here, :] - de)
        no[here, :] = on * (n[here, :] - dn)
        wo[here, :] = ou * (w[here, :] - du)
        po[here, :] = p
        return 0

    lax.fori_loop(0, 8, one, 0)


def tables():
    i = np.arange(NY)
    angle = 2 * np.pi * ((i[:, None] * i[None, :]) % NY) / NY
    hart = np.cos(angle) + np.sin(angle)
    k = np.arange(1, NZ + 1)
    sine = np.sin(np.pi * ((k[:, None] * k[None, :]) % (2 * (NZ + 1))) / (NZ + 1))
    lam = 4 * np.sin(np.pi * i / NY) ** 2
    mu = 4 * np.sin(np.pi * k / (2 * (NZ + 1))) ** 2

    def cut(a):
        hi = a.astype(np.float32).astype(BF16)
        return hi, (a - hi.astype(np.float64)).astype(np.float32).astype(BF16)

    lanes_of = np.arange(128)
    half = np.arange(NH)[:, None, None]
    who = np.arange(GZ)[None, :, None]
    lam = lam[half * LH + who * KL + lanes_of[None, None, :] % KL].reshape(NH * GZ, 128)
    packed = mu[(lanes_of[None, :] // KL) * 16 + np.arange(16)[:, None]]
    mu = np.repeat(mu[:, None], 128, 1)
    return (*cut(hart), *cut(sine), lam.astype(np.float32), mu.astype(np.float32), packed.astype(np.float32))


def local(east_velocity, north_velocity, upward_velocity, obstacle):
    e, n, w, o = (a.reshape(ROWS, NY) for a in (east_velocity, north_velocity, upward_velocity, obstacle))
    consts = [jnp.asarray(t) for t in tables()]
    any_spec = pl.BlockSpec(memory_space=pl.ANY)
    vmem = pl.BlockSpec(memory_space=pltpu.VMEM)
    ext = jax.ShapeDtypeStruct((ROWS + 16, NY), F32)
    planes = jax.ShapeDtypeStruct((2 * XR, NY), F32)

    def v(*shape, dtype=F32):
        return pltpu.VMEM(shape, dtype)

    dma = pltpu.SemaphoreType.DMA
    p, f, src, zp, zf = pl.pallas_call(
        main_kernel,
        out_shape=[ext, ext, jax.ShapeDtypeStruct((ROWS, NY), F32), planes, planes],
        in_specs=[any_spec] * 11,
        out_specs=[vmem] * 5,
        scratch_shapes=[
            v(ROWS + 8, NY), v(ROWS, NY), v(ROWS, NY), v(ROWS, NY, dtype=jnp.int32),
            v(NY, NY, dtype=BF16), v(NY, NY, dtype=BF16), v(NZ, NZ, dtype=BF16), v(NZ, NZ, dtype=BF16),
            v(NH * GZ, 128), v(NZ, 128), v(16, 128),
            v(XR, NY), v(3 * XR, NY), v(2 * XR, NY),
            v(ROWS, LH), v(NH * NZ, W), v(NH * NZ, W), v(NZ, W, dtype=BF16), v(NZ, W, dtype=BF16),
            v(NH * NZ, W), v(NH * NZ, 128), v(NH * NZ, 128), v(NH * NZ, 128), v(NH * NZ, 128),
            v(NH * XY * 32, 128), v(32, 128), v(NH * NZ, W), v(NH * NZ, W), v(ROWS, LH),
            dma((11,)), dma((6,)), dma((6,)), dma((NH,)), dma((NH,)), dma((NH,)), dma((NH,)),
            dma((NH,)), dma((NH,)), dma((4,)), dma((4,)),
        ],
        compiler_params=pltpu.CompilerParams(
            collective_id=0, has_side_effects=True, vmem_limit_bytes=40 * 1024 * 1024
        ),
        name="main",
    )(e, n, w, o, *consts)

    block = pl.BlockSpec((64, NY), lambda i: (i, 0))
    out = jax.ShapeDtypeStruct((ROWS, NY), F32)
    outs = pl.pallas_call(
        last_kernel,
        grid=(ROWS // 64,),
        out_shape=[out] * 5,
        in_specs=[block] * 4 + [pl.BlockSpec(a.shape, lambda i: (0, 0)) for a in (p, f, zp, zf)],
        out_specs=[block] * 5,
        compiler_params=pltpu.CompilerParams(vmem_limit_bytes=24 * 1024 * 1024),
        name="last",
    )(e, n, w, src, p, f, zp, zf)
    return tuple(a.reshape(XR, CZ, NY) for a in outs)


def solution(mesh):
    spec = P("xy", "gz", None)
    return jax.shard_map(local, mesh=mesh, in_specs=(spec,) * 4, out_specs=(spec,) * 5, check_vma=False)
```

```python
import functools

import jax
import jax.numpy as jnp
import numpy as np
from jax import lax
from jax.experimental import pallas as pl
from jax.experimental.pallas import tpu as pltpu
from jax.sharding import PartitionSpec as P

NX = 512
NY = 512
NZ = 256
GZ = 32
XY = 8
XR = NX // XY
CZ = NZ // GZ
NH = 2
KL = NY // GZ // NH
XL = 128 // KL
J = XR // XL
LH = NY // NH
W = J * 128
ROWS = XR * CZ
LOGJ = J.bit_length() - 1
BR = 32
F32 = jnp.float32
BF16 = jnp.bfloat16


def split(a):
    hi = a.astype(BF16)
    return hi, (a - hi.astype(F32)).astype(BF16)


def dot(a, b):
    return jnp.dot(a, b, preferred_element_type=F32)


def dot3(a, b):
    return dot(a[0], b[0]) + (dot(a[0], b[1]) + dot(a[1], b[0]))


def lanes(shape):
    return lax.broadcasted_iota(jnp.int32, shape, 1)


def roll(a, shift):
    return pltpu.roll(a, shift % 128, 1)


def exchange_lanes(tiles):
    tiles = list(tiles)
    group = lanes((8, 128)) // KL
    step = 1
    while step < XL:
        clear = (group & step) == 0
        for i in range(XL):
            if not i & step:
                k = i | step
                a, b = tiles[i], tiles[k]
                tiles[i] = jnp.where(clear, a, roll(b, step * KL))
                tiles[k] = jnp.where(clear, roll(a, -step * KL), b)
        step *= 2
    return tiles


def main_kernel(
    e_h, n_h, w_h, o_h, hh_h, hl_h, sh_h, sl_h, lam_h, mu_h, mup_h,
    p_v, f_v, src_v, zp_v, zf_v, e_v, n_v, w_v,
    o_v, hh, hl, sh, sl, lam, mu, mup,
    wa_v, zs_v, zps_v, y_v, send1, recv1, dh, dl, x_v, ea_v, eb_v, r_v, c_v, ag_v, uv_v, send2, recv2, zz_v,
    load_sem, halo_s, halo_r, a_s, a_r, g_s, g_r, b_s, b_r, ph_s, ph_r,
):
    me = lax.axis_index("gz")
    xi = lax.axis_index("xy")

    def gz(o):
        return {"gz": lax.rem(me + o, GZ)}

    def xy(o):
        return {"xy": lax.rem(xi + o, XY)}

    def load(k, src, dst):
        copy = pltpu.make_async_copy(src, dst, load_sem.at[k])
        copy.start()
        return copy

    def remote(src, dst, ssem, rsem, who):
        copy = pltpu.make_async_remote_copy(
            src_ref=src, dst_ref=dst, send_sem=ssem, recv_sem=rsem, device_id=who,
            device_id_type=pl.DeviceIdType.MESH,
        )
        copy.start()
        return copy

    loads = [
        load(0, o_h, o_v),
        load(1, w_h, w_v),
        load(2, e_h, e_v.at[pl.ds(0, ROWS)]),
        load(3, n_h, n_v),
        load(4, hh_h, hh),
        load(5, hl_h, hl),
        load(6, sh_h, sh),
        load(7, sl_h, sl),
        load(8, lam_h, lam),
        load(9, mu_h, mu),
        load(10, mup_h, mup),
    ]

    barrier = pltpu.get_barrier_semaphore()

    def greet_gz(o, _):
        pl.semaphore_signal(barrier, inc=1, device_id=gz(o), device_id_type=pl.DeviceIdType.MESH)
        return 0

    def greet_xy(o, _):
        pl.semaphore_signal(barrier, inc=1, device_id=xy(o), device_id_type=pl.DeviceIdType.MESH)
        return 0

    lax.fori_loop(1, GZ, greet_gz, 0)
    lax.fori_loop(1, XY, greet_xy, 0)

    with jax.named_scope("fluid"):
        loads[0].wait()

        def to_fluid(i, _):
            rows = pl.ds(pl.multiple_of(i * 64, 64), 64)
            f_v[pl.ds(pl.multiple_of(8 + i * 64, 8), 64), :] = (1 - o_v[rows, :]).astype(F32)
            return 0

        lax.fori_loop(0, ROWS // 64, to_fluid, 0)
        loads[1].wait()
        loads[2].wait()

        def edge(i, _):
            for k in range(8):
                x = i * 8 + k
                zs_v[pl.ds(x, 1), :] = f_v[pl.ds(x * 8 + 15, 1), :]
                zs_v[pl.ds(XR + x, 1), :] = f_v[pl.ds(x * 8 + 8, 1), :]
                zs_v[pl.ds(2 * XR + x, 1), :] = w_v[pl.ds(x * 8, 1), :]
            return 0

        lax.fori_loop(0, XR // 8, edge, 0)
    with jax.named_scope("barrier"):
        pl.semaphore_wait(barrier, GZ - 1 + XY - 1)
    halos = [
        remote(zs_v.at[pl.ds(2 * XR, XR)], wa_v, halo_s.at[0], halo_r.at[0], gz(GZ - 1)),
        remote(zs_v.at[pl.ds(XR, XR)], zf_v.at[pl.ds(XR, XR)], halo_s.at[1], halo_r.at[1], gz(GZ - 1)),
        remote(zs_v.at[pl.ds(0, XR)], zf_v.at[pl.ds(0, XR)], halo_s.at[2], halo_r.at[2], gz(1)),
        remote(f_v.at[pl.ds(ROWS, 8)], f_v.at[pl.ds(0, 8)], halo_s.at[3], halo_r.at[3], xy(1)),
        remote(f_v.at[pl.ds(8, 8)], f_v.at[pl.ds(ROWS + 8, 8)], halo_s.at[4], halo_r.at[4], xy(XY - 1)),
        remote(e_v.at[pl.ds(0, 8)], e_v.at[pl.ds(ROWS, 8)], halo_s.at[5], halo_r.at[5], xy(XY - 1)),
    ]
    with jax.named_scope("waithalo"):
        loads[3].wait()
        for k in range(4, 11):
            loads[k].wait()
        for h in halos:
            h.wait()

    sub = lax.broadcasted_iota(jnp.int32, (8, NY), 0)
    first = me == 0
    last = me == GZ - 1

    with jax.named_scope("source"):
        def source(i, _):
            base = pl.multiple_of(i * 8, 8)
            here = pl.ds(base, 8)
            f = f_v[pl.ds(pl.multiple_of(base + 8, 8), 8), :]
            fw = f_v[here, :]
            fe = f_v[pl.ds(pl.multiple_of(base + 16, 8), 8), :]
            east = f * (fw * e_v[here, :] - fe * e_v[pl.ds(pl.multiple_of(base + 8, 8), 8), :])
            fn = f * pltpu.roll(f, 1, 1) * n_v[here, :]
            north = fn - pltpu.roll(fn, NY - 1, 1)
            w = w_v[here, :]
            below = jnp.broadcast_to(zf_v[pl.ds(i, 1), :], (8, NY))
            above = jnp.broadcast_to(zf_v[pl.ds(XR + i, 1), :], (8, NY))
            wabove = jnp.broadcast_to(wa_v[pl.ds(i, 1), :], (8, NY))
            below = jnp.where(first, 1.0, below)
            above = jnp.where(last, 0.0, above)
            fb = jnp.where(sub == 0, below, pltpu.roll(f, 1, 0))
            fa = jnp.where(sub == 7, above, pltpu.roll(f, 7, 0))
            wn = jnp.where(sub == 7, wabove, pltpu.roll(w, 7, 0))
            up = f * (fb * w - fa * wn)
            src_v[here, :] = east + north + up
            return 0

        lax.fori_loop(0, XR, source, 0, unroll=4)

    def wait_bytes(ref, sem):
        pltpu.make_async_copy(ref, ref, sem).wait()

    for h in range(NH):
        hcol = pl.ds(h * LH, LH)

        with jax.named_scope("forward"):
            def forward(i, _):
                rows = pl.ds(pl.multiple_of(i * 256, 256), 256)
                y_v[rows, :] = dot3(split(src_v[rows, :]), (hh[:, hcol], hl[:, hcol]))
                return 0

            lax.fori_loop(0, ROWS // 256, forward, 0)

        with jax.named_scope("pack"):
            def pack(j, _):
                for t in range(LH // 128):
                    tiles = exchange_lanes(
                        [y_v[pl.ds(pl.multiple_of((x * J + j) * 8, 8), 8), pl.ds(t * 128, 128)] for x in range(XL)]
                    )
                    for a in range(XL):
                        send1[pl.ds((h * GZ + t * XL + a) * 8, 8), pl.ds(pl.multiple_of(j * 128, 128), 128)] = tiles[a]
                return 0

            lax.fori_loop(0, J, pack, 0)

        with jax.named_scope("send"):
            mine = pl.ds(pl.multiple_of(h * NZ + me * 8, 8), 8)

            def go(o, _):
                to = lax.rem(me + o, GZ)
                remote(
                    send1.at[pl.ds(pl.multiple_of((h * GZ + to) * 8, 8), 8)], recv1.at[mine],
                    a_s.at[h], a_r.at[h], {"gz": to},
                )
                return 0

            lax.fori_loop(1, GZ, go, 0)
            recv1[mine, :] = send1[pl.ds(pl.multiple_of((h * GZ + me) * 8, 8), 8), :]

    for h in range(NH):
        with jax.named_scope("rates"):
            lrow = lam[pl.ds(h * GZ + me, 1), :]

            def rates(i, _):
                rows = pl.ds(pl.multiple_of(i * 16, 16), 16)
                out = pl.ds(pl.multiple_of(h * NZ + i * 16, 16), 16)
                g = mu[rows, :] + lrow
                root = jnp.sqrt(g + 0.25 * g * g)
                r_v[out, :] = 1.0 / (1.0 + 0.5 * g + root)
                c_v[out, :] = (1.0 / (NZ + 1) / NY) / root
                return 0

            lax.fori_loop(0, NZ // 16, rates, 0)

    group = lanes((16, 128)) // KL
    wide = lanes((BR, 128)) // KL
    home = (lax.broadcasted_iota(jnp.int32, (BR, 128), 0) // 16) - wide

    for h in range(NH):
        with jax.named_scope("waita2a"):
            wait_bytes(recv1.at[pl.ds(h * NZ, NZ - 8)], a_r.at[h])

        with jax.named_scope("dst"):
            def cut(i, _):
                rows = pl.ds(pl.multiple_of(i * 16, 16), 16)
                a, b = split(recv1[pl.ds(pl.multiple_of(h * NZ + i * 16, 16), 16), :])
                dh[rows, :] = a
                dl[rows, :] = b
                return 0

            lax.fori_loop(0, NZ // 16, cut, 0)
            for c in range(W // 256):
                col = pl.ds(c * 256, 256)
                x_v[pl.ds(h * NZ, NZ), col] = dot3((sh[...], sl[...]), (dh[:, col], dl[:, col]))

        with jax.named_scope("sums"):
            def sums(i, carry):
                pa, pb = carry
                rows = pl.ds(pl.multiple_of(h * NZ + i * BR, BR), BR)
                r = r_v[rows, :]
                s = [x_v[rows, pl.ds(j * 128, 128)] for j in range(J)]
                u = [s[0]]
                for j in range(1, J):
                    u.append(s[j] + r * u[-1])
                v = [s[-1]]
                for j in range(J - 2, -1, -1):
                    v.append(s[j] + r * v[-1])
                v = v[::-1]
                for j in range(J):
                    x_v[rows, pl.ds(j * 128, 128)] = u[j] + v[j] - s[j]
                a, b = u[-1], v[0]
                pw = r
                for _ in range(LOGJ):
                    pw = pw * pw
                step = 1
                while step < XL:
                    a = a + jnp.where(wide >= step, pw * roll(a, step * KL), 0.0)
                    b = b + jnp.where(wide < XL - step, pw * roll(b, -step * KL), 0.0)
                    pw = pw * pw
                    step *= 2
                ea_v[rows, :] = jnp.where(wide >= 1, roll(a, KL), 0.0)
                eb_v[rows, :] = jnp.where(wide < XL - 1, roll(b, -KL), 0.0)
                for k in range(BR // 16):
                    q = i * (BR // 16) + k
                    at = group == q
                    cut16 = slice(k * 16, k * 16 + 16)
                    pa = jnp.where(at, pltpu.roll(a[cut16], lax.rem((q + 1) * KL, 128), 1), pa)
                    pb = jnp.where(at, pltpu.roll(b[cut16], q * KL, 1), pb)
                return pa, pb

            zero = jnp.zeros((16, 128), F32)
            pa, pb = lax.fori_loop(0, NZ // BR, sums, (zero, zero))
        with jax.named_scope("gather"):
            own = pl.ds(pl.multiple_of((h * XY + xi) * 32, 32), 32)
            ag_v[pl.ds(pl.multiple_of((h * XY + xi) * 32, 32), 16), :] = pa
            ag_v[pl.ds(pl.multiple_of((h * XY + xi) * 32 + 16, 16), 16), :] = pb

            def spread(o, _):
                remote(ag_v.at[own], ag_v.at[own], g_s.at[h], g_r.at[h], xy(o))
                return 0

            lax.fori_loop(1, XY, spread, 0)

    for h in range(NH):
        with jax.named_scope("waitgather"):
            wait_bytes(ag_v.at[pl.ds(h * XY * 32, (XY - 1) * 32)], g_r.at[h])
        with jax.named_scope("carry"):
            g = mup[...] + lam[pl.ds(h * GZ + me, 1), :]
            rp = 1.0 / (1.0 + 0.5 * g + jnp.sqrt(g + 0.25 * g * g))
            for _ in range(XR.bit_length() - 1):
                rp = rp * rp
            full = rp
            for _ in range(XY.bit_length() - 1):
                full = full * full
            close = 1.0 / (1.0 - full)

            def piece(o, part):
                at = (h * XY + lax.rem(xi + o, XY)) * 32 + part * 16
                return ag_v[pl.ds(pl.multiple_of(at, 16), 16), :]

            un, vn = piece(0, 0), piece(0, 1)
            for o in range(1, XY):
                un = un * rp + piece(o, 0)
                vn = vn * rp + piece(XY - o, 1)
            un = un * close
            vn = vn * close

        with jax.named_scope("finish"):
            def finish(i, _):
                rows = pl.ds(pl.multiple_of(h * NZ + i * BR, BR), BR)
                out = pl.ds(pl.multiple_of(i * BR, BR), BR)
                at = home == -(i * (BR // 16))
                ub = jnp.where(at, jnp.concatenate([un] * (BR // 16), 0), 0.0)
                vb = jnp.where(at, jnp.concatenate([vn] * (BR // 16), 0), 0.0)
                step = 1
                while step < XL:
                    ub = ub + roll(ub, step * KL)
                    vb = vb + roll(vb, step * KL)
                    step *= 2
                r = r_v[rows, :]
                powers = [r]
                for _ in range(J - 1):
                    powers.append(powers[-1] * r)
                pw = powers[-1]
                up = jnp.ones_like(r)
                down = jnp.ones_like(r)
                step = 1
                while step < XL:
                    on = (wide & step) != 0
                    up = jnp.where(on, up * pw, up)
                    down = jnp.where(on, down, down * pw)
                    pw = pw * pw
                    step *= 2
                cu = ea_v[rows, :] + up * ub
                cv = eb_v[rows, :] + down * vb
                c = c_v[rows, :]
                for j in range(J):
                    col = pl.ds(j * 128, 128)
                    sol = c * (x_v[rows, col] + powers[j] * cu + powers[J - 1 - j] * cv)
                    a, b = split(sol)
                    dh[out, col] = a
                    dl[out, col] = b
                return 0

            lax.fori_loop(0, NZ // BR, finish, 0)
        with jax.named_scope("idst"):
            for c in range(W // 256):
                col = pl.ds(c * 256, 256)
                send2[pl.ds(h * NZ, NZ), col] = dot3((sh[...], sl[...]), (dh[:, col], dl[:, col]))

        with jax.named_scope("back"):
            mine = pl.ds(pl.multiple_of((h * GZ + me) * 8, 8), 8)

            def back(o, _):
                to = lax.rem(me + o, GZ)
                remote(
                    send2.at[pl.ds(pl.multiple_of(h * NZ + to * 8, 8), 8)], recv2.at[mine],
                    b_s.at[h], b_r.at[h], {"gz": to},
                )
                return 0

            lax.fori_loop(1, GZ, back, 0)
            recv2[mine, :] = send2[pl.ds(pl.multiple_of(h * NZ + me * 8, 8), 8), :]

    for h in range(NH):
        with jax.named_scope("waitback"):
            wait_bytes(recv2.at[pl.ds(h * NZ, NZ - 8)], b_r.at[h])

        with jax.named_scope("unpack"):
            def unpack(j, _):
                for t in range(LH // 128):
                    tiles = exchange_lanes(
                        [
                            recv2[pl.ds((h * GZ + t * XL + a) * 8, 8), pl.ds(pl.multiple_of(j * 128, 128), 128)]
                            for a in range(XL)
                        ]
                    )
                    for x in range(XL):
                        zz_v[pl.ds(pl.multiple_of((x * J + j) * 8, 8), 8), pl.ds(t * 128, 128)] = tiles[x]
                return 0

            lax.fori_loop(0, J, unpack, 0)

        with jax.named_scope("inverse"):
            def inverse(i, _):
                rows = pl.ds(pl.multiple_of(i * 256, 256), 256)
                out = pl.ds(pl.multiple_of(8 + i * 256, 8), 256)
                hrow = pl.ds(h * LH, LH)
                part = dot3(split(zz_v[rows, :]), (hh[hrow, :], hl[hrow, :]))
                p_v[out, :] = part if h == 0 else p_v[out, :] + part
                return 0

            lax.fori_loop(0, ROWS // 256, inverse, 0)

    with jax.named_scope("pplanes"):
        def pedge(i, _):
            for k in range(8):
                x = i * 8 + k
                zps_v[pl.ds(x, 1), :] = p_v[pl.ds(x * 8 + 15, 1), :]
                zps_v[pl.ds(XR + x, 1), :] = p_v[pl.ds(x * 8 + 8, 1), :]
            return 0

        lax.fori_loop(0, XR // 8, pedge, 0)
        planes = [
            remote(zps_v.at[pl.ds(0, XR)], zp_v.at[pl.ds(0, XR)], ph_s.at[0], ph_r.at[0], gz(1)),
            remote(zps_v.at[pl.ds(XR, XR)], zp_v.at[pl.ds(XR, XR)], ph_s.at[1], ph_r.at[1], gz(GZ - 1)),
            remote(p_v.at[pl.ds(ROWS, 8)], p_v.at[pl.ds(0, 8)], ph_s.at[2], ph_r.at[2], xy(1)),
            remote(p_v.at[pl.ds(8, 8)], p_v.at[pl.ds(ROWS + 8, 8)], ph_s.at[3], ph_r.at[3], xy(XY - 1)),
        ]
    with jax.named_scope("waitend"):
        for h in range(NH):
            wait_bytes(send1.at[pl.ds(h * NZ, NZ - 8)], a_s.at[h])
            wait_bytes(ag_v.at[pl.ds(h * XY * 32, (XY - 1) * 32)], g_s.at[h])
            wait_bytes(send2.at[pl.ds(h * NZ, NZ - 8)], b_s.at[h])
        for c in planes:
            c.wait()


def last_kernel(e, n, w, src, p_v, f_v, zp, zf, eo, no, wo, po, ro):
    step = pl.program_id(0)
    me = lax.axis_index("gz")
    first = me == 0
    last = me == GZ - 1
    sub = lax.broadcasted_iota(jnp.int32, (8, NY), 0)

    def one(i, _):
        here = pl.ds(pl.multiple_of(i * 8, 8), 8)
        x = step * 8 + i
        base = pl.multiple_of(x * 8, 8)
        mid = pl.ds(pl.multiple_of(base + 8, 8), 8)
        east = pl.ds(pl.multiple_of(base + 16, 8), 8)
        p = p_v[mid, :]
        f = f_v[mid, :]
        below = jnp.where(first, 1.0, jnp.broadcast_to(zf[pl.ds(x, 1), :], (8, NY)))
        above = jnp.where(last, 0.0, jnp.broadcast_to(zf[pl.ds(XR + x, 1), :], (8, NY)))
        pbelow = jnp.where(first, 0.0, jnp.broadcast_to(zp[pl.ds(x, 1), :], (8, NY)))
        pabove = jnp.broadcast_to(zp[pl.ds(XR + x, 1), :], (8, NY))
        oe = f * f_v[pl.ds(base, 8), :]
        oe_next = f * f_v[east, :]
        on = f * pltpu.roll(f, 1, 1)
        on_next = pltpu.roll(on, NY - 1, 1)
        ou = f * jnp.where(sub == 0, below, pltpu.roll(f, 1, 0))
        ou_next = f * jnp.where(sub == 7, above, pltpu.roll(f, 7, 0))
        de = p - p_v[pl.ds(base, 8), :]
        de_next = p - p_v[east, :]
        dn = p - pltpu.roll(p, 1, 1)
        dn_next = p - pltpu.roll(p, NY - 1, 1)
        du = p - jnp.where(sub == 0, pbelow, pltpu.roll(p, 1, 0))
        du_next = p - jnp.where(sub == 7, pabove, pltpu.roll(p, 7, 0))
        applied = oe * de + oe_next * de_next + on * dn + on_next * dn_next + ou * du + ou_next * du_next
        ro[here, :] = src[here, :] - applied
        eo[here, :] = oe * (e[here, :] - de)
        no[here, :] = on * (n[here, :] - dn)
        wo[here, :] = ou * (w[here, :] - du)
        po[here, :] = p
        return 0

    lax.fori_loop(0, 8, one, 0, unroll=4)


def tables():
    i = np.arange(NY)
    angle = 2 * np.pi * ((i[:, None] * i[None, :]) % NY) / NY
    hart = np.cos(angle) + np.sin(angle)
    k = np.arange(1, NZ + 1)
    sine = np.sin(np.pi * ((k[:, None] * k[None, :]) % (2 * (NZ + 1))) / (NZ + 1))
    lam = 4 * np.sin(np.pi * i / NY) ** 2
    mu = 4 * np.sin(np.pi * k / (2 * (NZ + 1))) ** 2

    def cut(a):
        hi = a.astype(np.float32).astype(BF16)
        return hi, (a - hi.astype(np.float64)).astype(np.float32).astype(BF16)

    lanes_of = np.arange(128)
    half = np.arange(NH)[:, None, None]
    who = np.arange(GZ)[None, :, None]
    lam = lam[half * LH + who * KL + lanes_of[None, None, :] % KL].reshape(NH * GZ, 128)
    packed = mu[(lanes_of[None, :] // KL) * 16 + np.arange(16)[:, None]]
    mu = np.repeat(mu[:, None], 128, 1)
    return (*cut(hart), *cut(sine), lam.astype(np.float32), mu.astype(np.float32), packed.astype(np.float32))


def local(east_velocity, north_velocity, upward_velocity, obstacle):
    fields = (east_velocity, north_velocity, upward_velocity, obstacle)
    args = [pltpu.with_memory_space_constraint(a.reshape(ROWS, NY), pltpu.HBM) for a in fields]
    args += [pltpu.with_memory_space_constraint(jnp.asarray(t), pltpu.HBM) for t in tables()]
    any_spec = pl.BlockSpec(memory_space=pl.ANY)
    vmem = pl.BlockSpec(memory_space=pltpu.VMEM)
    ext = jax.ShapeDtypeStruct((ROWS + 16, NY), F32)
    planes = jax.ShapeDtypeStruct((2 * XR, NY), F32)

    def v(*shape, dtype=F32):
        return pltpu.VMEM(shape, dtype)

    dma = pltpu.SemaphoreType.DMA
    field = jax.ShapeDtypeStruct((ROWS, NY), F32)
    longer = jax.ShapeDtypeStruct((ROWS + 8, NY), F32)
    p, f, src, zp, zf, e, n, w = pl.pallas_call(
        main_kernel,
        out_shape=[ext, ext, field, planes, planes, longer, field, field],
        in_specs=[any_spec] * 11,
        out_specs=[vmem] * 8,
        scratch_shapes=[
            v(ROWS, NY, dtype=jnp.int32),
            v(NY, NY, dtype=BF16), v(NY, NY, dtype=BF16), v(NZ, NZ, dtype=BF16), v(NZ, NZ, dtype=BF16),
            v(NH * GZ, 128), v(NZ, 128), v(16, 128),
            v(XR, NY), v(3 * XR, NY), v(2 * XR, NY),
            v(ROWS, LH), v(NH * NZ, W), v(NH * NZ, W), v(NZ, W, dtype=BF16), v(NZ, W, dtype=BF16),
            v(NH * NZ, W), v(NH * NZ, 128), v(NH * NZ, 128), v(NH * NZ, 128), v(NH * NZ, 128),
            v(NH * XY * 32, 128), v(32, 128), v(NH * NZ, W), v(NH * NZ, W), v(ROWS, LH),
            dma((11,)), dma((6,)), dma((6,)), dma((NH,)), dma((NH,)), dma((NH,)), dma((NH,)),
            dma((NH,)), dma((NH,)), dma((4,)), dma((4,)),
        ],
        compiler_params=pltpu.CompilerParams(
            collective_id=0, has_side_effects=True, vmem_limit_bytes=32 * 1024 * 1024
        ),
        name="main",
    )(*args)

    block = pl.BlockSpec((64, NY), lambda i: (i, 0))
    outs = pl.pallas_call(
        last_kernel,
        grid=(ROWS // 64,),
        out_shape=[field] * 5,
        in_specs=[block] * 4 + [pl.BlockSpec(a.shape, lambda i: (0, 0)) for a in (p, f, zp, zf)],
        out_specs=[block] * 5,
        compiler_params=pltpu.CompilerParams(vmem_limit_bytes=16 * 1024 * 1024),
        name="last",
    )(e, n, w, src, p, f, zp, zf)
    return tuple(a.reshape(XR, CZ, NY) for a in outs)


def solution(mesh):
    spec = P("xy", "gz", None)
    return jax.shard_map(local, mesh=mesh, in_specs=(spec,) * 4, out_specs=(spec,) * 5, check_vma=False)
```

```python
import functools

import jax
import jax.numpy as jnp
import numpy as np
from jax import lax
from jax.experimental import pallas as pl
from jax.experimental.pallas import tpu as pltpu
from jax.sharding import PartitionSpec as P

NX = 512
NY = 512
NZ = 256
GZ = 32
XY = 8
XR = NX // XY
CZ = NZ // GZ
NH = 4
KL = NY // GZ // NH
XL = 128 // KL
J = XR // XL
LH = NY // NH
W = J * 128
ROWS = XR * CZ
LOGJ = J.bit_length() - 1
BR = 32
BW = 128
NG = LH // 128
PR = NZ // XL
LAG = 2
XS = 16
EDGE = 2 * XR + 16
F32 = jnp.float32
BF16 = jnp.bfloat16


def split(a):
    hi = a.astype(BF16)
    return hi, (a - hi.astype(F32)).astype(BF16)


def dot(a, b):
    return jnp.dot(a, b, preferred_element_type=F32)


def dot3(a, b):
    return dot(a[0], b[0]) + (dot(a[0], b[1]) + dot(a[1], b[0]))


def lanes(shape):
    return lax.broadcasted_iota(jnp.int32, shape, 1)


def slot(t):
    return t % NG * XL + t // NG


def far_first():
    hops = (0, 1, 2, 1)
    every = [(x, y, c) for x in range(4) for y in range(4) for c in range(2)]
    every.remove((0, 0, 0))
    return sorted(every, key=lambda o: -(hops[o[0]] + hops[o[1]]))


def roll(a, shift):
    return pltpu.roll(a, shift % 128, 1)


def exchange_lanes(tiles):
    tiles = list(tiles)
    group = lanes((8, 128)) // KL
    step = 1
    while step < XL:
        clear = (group & step) == 0
        for i in range(XL):
            if not i & step:
                k = i | step
                a, b = tiles[i], tiles[k]
                tiles[i] = jnp.where(clear, a, roll(b, step * KL))
                tiles[k] = jnp.where(clear, roll(a, -step * KL), b)
        step *= 2
    return tiles


def row(ref, r):
    return jnp.broadcast_to(ref[pl.ds(r, 1), :], (8, ref.shape[1]))


def tile8(at):
    return pl.ds(pl.multiple_of(at * 8, 8), 8)


def main_kernel(
    e_h, n_h, w_h, o_h, hh_h, hl_h, sh_h, sl_h, lam_h, mu_h, mup_h,
    p_v, eo_v, no_v, wo_v, ro_v, z0_v, z7_v,
    f_v, e_v, n_v, w_v, zp_v, zf_v, ga_v, px_v,
    o_v, src_v, hh, hl, sh, sl, lam, mu, mup,
    zs_v, gs_v, fx_v, ex_v, cc_v, cy_v, zb_v, pb_v, up_v, dn_v,
    y_v, send1, recv1, dh, dl, x_v, ea_v, eb_v, r_v, c_v, ag_v, send2, recv2, zz_v,
    load_sem, halo_s, halo_r, a_s, a_r, g_s, g_r, b_s, b_r, ph_s, ph_r,
):
    me = lax.axis_index("gz")
    xi = lax.axis_index("xy")
    first = me == 0
    last = me == GZ - 1
    spot = lax.rem(me, NG) * XL + me // NG

    def gz(o):
        return {"gz": lax.rem(me + o, GZ)}

    def xy(o):
        return {"xy": lax.rem(xi + o, XY)}

    def peer(o):
        x = lax.rem(me // 8 + o[0], 4)
        y = lax.rem(me // 2 + o[1], 4)
        return (x * 4 + y) * 2 + lax.rem(me + o[2], 2)

    def load(k, src, dst):
        copy = pltpu.make_async_copy(src, dst, load_sem.at[k])
        copy.start()
        return copy

    def remote(src, dst, ssem, rsem, who):
        copy = pltpu.make_async_remote_copy(
            src_ref=src, dst_ref=dst, send_sem=ssem, recv_sem=rsem, device_id=who,
            device_id_type=pl.DeviceIdType.MESH,
        )
        copy.start()
        return copy

    def wait_bytes(ref, sem):
        pltpu.make_async_copy(ref, ref, sem).wait()

    flags = load(0, o_h, o_v)
    barrier = pltpu.get_barrier_semaphore()

    def greet_gz(o, _):
        pl.semaphore_signal(barrier, inc=1, device_id=gz(o), device_id_type=pl.DeviceIdType.MESH)
        return 0

    def greet_xy(o, _):
        pl.semaphore_signal(barrier, inc=1, device_id=xy(o), device_id_type=pl.DeviceIdType.MESH)
        return 0

    lax.fori_loop(1, GZ, greet_gz, 0)
    lax.fori_loop(1, XY, greet_xy, 0)

    loads = [
        flags,
        load(1, w_h, w_v),
        load(2, e_h, e_v.at[pl.ds(0, ROWS)]),
        load(3, n_h, n_v),
        load(4, hh_h, hh),
        load(5, hl_h, hl),
        load(6, sh_h, sh),
        load(7, sl_h, sl),
        load(8, lam_h, lam),
        load(9, mu_h, mu),
        load(10, mup_h, mup),
    ]

    with jax.named_scope("fluid"):
        loads[0].wait()

        def to_fluid(i, _):
            rows = pl.ds(pl.multiple_of(i * 64, 64), 64)
            f_v[pl.ds(pl.multiple_of(8 + i * 64, 8), 64), :] = (1 - o_v[rows, :]).astype(F32)
            return 0

        lax.fori_loop(0, ROWS // 64, to_fluid, 0)
        f_v[pl.ds(0, 8), :] = jnp.zeros((8, NY), F32)
        f_v[pl.ds(ROWS + 8, 8), :] = jnp.zeros((8, NY), F32)
        e_v[pl.ds(ROWS, 8), :] = jnp.zeros((8, NY), F32)
        loads[1].wait()

        def edge(i, _):
            for k in range(8):
                x = i * 8 + k
                low = f_v[pl.ds(x * 8 + 8, 1), :]
                zs_v[pl.ds(x, 1), :] = f_v[pl.ds(x * 8 + 15, 1), :]
                zs_v[pl.ds(XR + x, 1), :] = low
                gs_v[pl.ds(x, 1), :] = low * w_v[pl.ds(x * 8, 1), :]
            return 0

        lax.fori_loop(0, XR // 8, edge, 0)
        loads[2].wait()
    with jax.named_scope("barrier"):
        pl.semaphore_wait(barrier, GZ - 1 + XY - 1)
    halos = [
        remote(gs_v, ga_v, halo_s.at[0], halo_r.at[0], gz(GZ - 1)),
        remote(zs_v.at[pl.ds(0, XR)], zf_v.at[pl.ds(0, XR)], halo_s.at[1], halo_r.at[1], gz(1)),
        remote(f_v.at[pl.ds(ROWS, 8)], fx_v.at[pl.ds(0, 8)], halo_s.at[2], halo_r.at[2], xy(1)),
        remote(f_v.at[pl.ds(8, 8)], fx_v.at[pl.ds(8, 8)], halo_s.at[3], halo_r.at[3], xy(XY - 1)),
        remote(e_v.at[pl.ds(0, 8)], ex_v, halo_s.at[4], halo_r.at[4], xy(XY - 1)),
        remote(zs_v.at[pl.ds(XR, XR)], zf_v.at[pl.ds(XR, XR)], halo_s.at[5], halo_r.at[5], gz(GZ - 1)),
    ]

    with jax.named_scope("source"):
        loads[3].wait()
        sub = lax.broadcasted_iota(jnp.int32, (8, NY), 0)

        def source(i, _):
            def east(x):
                return f_v[tile8(x + 1), :] * f_v[tile8(x), :] * e_v[tile8(x), :]

            now = east(i * 8)
            for k in range(8):
                x = i * 8 + k
                then = east(x + 1)
                f = f_v[tile8(x + 1), :]
                north = f * pltpu.roll(f, 1, 1) * n_v[tile8(x), :]
                up = jnp.where(sub == 0, 0.0, f * pltpu.roll(f, 1, 0) * w_v[tile8(x), :])
                src_v[tile8(x), :] = (now - then) + (north - pltpu.roll(north, NY - 1, 1)) + (up - pltpu.roll(up, 7, 0))
                now = then
            return 0

        lax.fori_loop(0, XR // 8, source, 0)

    with jax.named_scope("forward"):
        for k in range(4, 11):
            loads[k].wait()

        def forward(i, _):
            y = dot3(split(src_v[pl.ds(pl.multiple_of(i * 128, 128), 128), :]), (hh[...], hl[...]))
            for h in range(NH):
                out = pl.ds(pl.multiple_of(h * ROWS + i * 128, 128), 128)
                y_v[out, :] = y[:, h * LH : h * LH + LH]
            return 0

        lax.fori_loop(0, ROWS // 128, forward, 0)

    with jax.named_scope("waithalo"):
        for h in halos[:5]:
            h.wait()

    with jax.named_scope("edges"):
        low, high = pl.ds(0, XR), pl.ds(XR, XR)
        cc_v[low, :] = jnp.where(first, 1.0, zf_v[low, :]) * gs_v[...]
        cc_v[high, :] = jnp.where(last, 0.0, zs_v[low, :] * ga_v[...] * -1.0)
        cc_v[pl.ds(2 * XR, 8), :] = fx_v[pl.ds(0, 8), :] * f_v[pl.ds(8, 8), :] * e_v[pl.ds(0, 8), :]
        cc_v[pl.ds(2 * XR + 8, 8), :] = f_v[pl.ds(ROWS, 8), :] * fx_v[pl.ds(8, 8), :] * ex_v[...] * -1.0
        cy = dot3(split(cc_v[...]), (hh[...], hl[...]))
        for h in range(NH):
            part = cy[:, h * LH : h * LH + LH]
            cy_v[h] = part
            lo, hi = pl.ds(h * ROWS, 8), pl.ds(h * ROWS + ROWS - 8, 8)
            y_v[lo, :] = y_v[lo, :] + part[2 * XR : 2 * XR + 8]
            y_v[hi, :] = y_v[hi, :] + part[2 * XR + 8 :]

    sub1 = lax.broadcasted_iota(jnp.int32, (8, 128), 0)
    for h in range(NH):
        with jax.named_scope("pack"):
            mine = pl.ds(pl.multiple_of(h * NZ + me * 8, 8), 8)
            for t in range(NG):
                tcol = pl.ds(t * 128, 128)

                for j in range(J):
                    tiles = []
                    for a in range(XL):
                        x = a * J + j
                        below = jnp.broadcast_to(cy_v[h, pl.ds(x, 1), tcol], (8, 128))
                        above = jnp.broadcast_to(cy_v[h, pl.ds(XR + x, 1), tcol], (8, 128))
                        extra = jnp.where(sub1 == 0, below, jnp.where(sub1 == 7, above, 0.0))
                        tiles.append(y_v[pl.ds((h * XR + x) * 8, 8), tcol] + extra)
                    tiles = exchange_lanes(tiles)
                    for a in range(XL):
                        send1[pl.ds((h * GZ + t * XL + a) * 8, 8), pl.ds(j * 128, 128)] = tiles[a]

            for o in far_first():
                to = peer(o)
                place = lax.rem(to, NG) * XL + to // NG
                remote(send1.at[tile8(h * GZ + place)], recv1.at[mine], a_s.at[h], a_r.at[h], {"gz": to})
            recv1[mine, :] = send1[tile8(h * GZ + spot), :]

    with jax.named_scope("rates"):
        group_r = lanes((64, 128)) // KL
        for h in range(NH):
            lrow = lam[pl.ds(h * GZ + me, 1), :]

            def rates(i, _):
                rows = pl.ds(pl.multiple_of(i * 64, 64), 64)
                out = pl.ds(pl.multiple_of(h * NZ + i * 64, 64), 64)
                g = mu[rows, :] + lrow
                root = jnp.sqrt(g + 0.25 * g * g)
                r = 1.0 / (1.0 + 0.5 * g + root)
                r_v[out, :] = r
                c_v[out, :] = (1.0 / (NZ + 1) / NY) / root
                pw = r
                for _ in range(LOGJ):
                    pw = pw * pw
                up = jnp.ones_like(r)
                down = jnp.ones_like(r)
                step = 1
                while step < XL:
                    on = (group_r & step) != 0
                    up = jnp.where(on, up * pw, up)
                    down = jnp.where(on, down, down * pw)
                    pw = pw * pw
                    step *= 2
                up_v[out, :] = up
                dn_v[out, :] = down
                return 0

            lax.fori_loop(0, NZ // 64, rates, 0)

    group = lanes((PR, 128)) // KL
    wide = lanes((BW, 128)) // KL
    home = lax.broadcasted_iota(jnp.int32, (BW, 128), 0) // PR - wide
    QS = BW // PR

    def descend(h):
        with jax.named_scope("waita2a"):
            wait_bytes(recv1.at[pl.ds(h * NZ, NZ - 8)], a_r.at[h])

        with jax.named_scope("dst"):
            def cut(i, _):
                rows = pl.ds(pl.multiple_of(i * 32, 32), 32)
                a, b = split(recv1[pl.ds(pl.multiple_of(h * NZ + i * 32, 32), 32), :])
                dh[rows, :] = a
                dl[rows, :] = b
                return 0

            lax.fori_loop(0, NZ // 32, cut, 0)
            for c in range(W // 256):
                col = pl.ds(c * 256, 256)
                x_v[pl.ds(h * NZ, NZ), col] = dot3((sh[...], sl[...]), (dh[:, col], dl[:, col]))

        with jax.named_scope("sums"):
            def sums(i, _):
                rows = pl.ds(pl.multiple_of(h * NZ + i * BR, BR), BR)
                r = r_v[rows, :]
                s = [x_v[rows, pl.ds(j * 128, 128)] for j in range(J)]
                u = [s[0]]
                for j in range(1, J):
                    u.append(s[j] + r * u[-1])
                v = [s[-1]]
                for j in range(J - 2, -1, -1):
                    v.append(s[j] + r * v[-1])
                v = v[::-1]
                for j in range(J):
                    x_v[rows, pl.ds(j * 128, 128)] = u[j] + v[j] - s[j]
                ea_v[rows, :] = u[-1]
                eb_v[rows, :] = v[0]
                return 0

            lax.fori_loop(0, NZ // BR, sums, 0)
            pa = jnp.zeros((PR, 128), F32)
            pb = jnp.zeros((PR, 128), F32)
            for i in range(NZ // BW):
                rows = pl.ds(h * NZ + i * BW, BW)
                a, b = ea_v[rows, :], eb_v[rows, :]
                pw = r_v[rows, :]
                for _ in range(LOGJ):
                    pw = pw * pw
                step = 1
                while step < XL:
                    a = a + jnp.where(wide >= step, pw * roll(a, step * KL), 0.0)
                    b = b + jnp.where(wide < XL - step, pw * roll(b, -step * KL), 0.0)
                    pw = pw * pw
                    step *= 2
                ea_v[rows, :] = jnp.where(wide >= 1, roll(a, KL), 0.0)
                eb_v[rows, :] = jnp.where(wide < XL - 1, roll(b, -KL), 0.0)
                for k in range(QS):
                    q = i * QS + k
                    piece = slice(k * PR, k * PR + PR)
                    pa = jnp.where(group == q, roll(a[piece], (q + 1) * KL), pa)
                    pb = jnp.where(group == q, roll(b[piece], q * KL), pb)

        with jax.named_scope("gather"):
            at = pl.multiple_of((h * XY + xi) * 2 * PR, 2 * PR)
            own = pl.ds(at, 2 * PR)
            ag_v[pl.ds(at, PR), :] = pa
            ag_v[pl.ds(pl.multiple_of(at + PR, PR), PR), :] = pb

            def spread(o, _):
                remote(ag_v.at[own], ag_v.at[own], g_s.at[h], g_r.at[h], xy(o))
                return 0

            lax.fori_loop(1, XY, spread, 0)

    def ascend(h):
        with jax.named_scope("waitgather"):
            wait_bytes(ag_v.at[pl.ds(h * XY * 2 * PR, (XY - 1) * 2 * PR)], g_r.at[h])
        with jax.named_scope("finish"):
            g = mup[...] + lam[pl.ds(h * GZ + me, 1), :]
            rp = 1.0 / (1.0 + 0.5 * g + jnp.sqrt(g + 0.25 * g * g))
            for _ in range(XR.bit_length() - 1):
                rp = rp * rp
            full = rp
            for _ in range(XY.bit_length() - 1):
                full = full * full
            close = 1.0 / (1.0 - full)

            def piece(o, part):
                at = (h * XY + lax.rem(xi + o, XY)) * 2 * PR + part * PR
                return ag_v[pl.ds(pl.multiple_of(at, PR), PR), :]

            un, vn = piece(0, 0), piece(0, 1)
            for o in range(1, XY):
                un = un * rp + piece(o, 0)
                vn = vn * rp + piece(XY - o, 1)
            un = un * close
            vn = vn * close

            for i in range(NZ // BW):
                rows = pl.ds(h * NZ + i * BW, BW)
                at = home == -(i * QS)
                ub = jnp.where(at, jnp.concatenate([un] * QS, 0), 0.0)
                vb = jnp.where(at, jnp.concatenate([vn] * QS, 0), 0.0)
                step = 1
                while step < XL:
                    ub = ub + roll(ub, step * KL)
                    vb = vb + roll(vb, step * KL)
                    step *= 2
                ea_v[rows, :] = ea_v[rows, :] + up_v[rows, :] * ub
                eb_v[rows, :] = eb_v[rows, :] + dn_v[rows, :] * vb

            def finish(i, _):
                rows = pl.ds(pl.multiple_of(h * NZ + i * BR, BR), BR)
                out = pl.ds(pl.multiple_of(i * BR, BR), BR)
                r = r_v[rows, :]
                c = c_v[rows, :]
                cu = [r * ea_v[rows, :]]
                cv = [r * eb_v[rows, :]]
                for _ in range(J - 1):
                    cu.append(r * cu[-1])
                    cv.append(r * cv[-1])
                for j in range(J):
                    col = pl.ds(j * 128, 128)
                    a, b = split(c * (x_v[rows, col] + cu[j] + cv[J - 1 - j]))
                    dh[out, col] = a
                    dl[out, col] = b
                return 0

            lax.fori_loop(0, NZ // BR, finish, 0)

        with jax.named_scope("idst"):
            for c in range(W // 256):
                col = pl.ds(c * 256, 256)
                send2[pl.ds(h * NZ, NZ), col] = dot3((sh[...], sl[...]), (dh[:, col], dl[:, col]))

        with jax.named_scope("back"):
            mine = tile8(h * GZ + spot)

            for o in far_first():
                to = peer(o)
                remote(send2.at[tile8(h * GZ + to)], recv2.at[mine], b_s.at[h], b_r.at[h], {"gz": to})
            recv2[mine, :] = send2[tile8(h * GZ + me), :]

    for k in range(NH + LAG):
        if k < NH:
            descend(k)
        if k >= LAG:
            ascend(k - LAG)

    for h in range(NH):
        hrow = pl.ds(h * LH, LH)
        with jax.named_scope("waitback"):
            wait_bytes(recv2.at[pl.ds(h * NZ, NZ - 8)], b_r.at[h])

        with jax.named_scope("unpack"):
            for t in range(NG):
                for j in range(J):
                    tiles = exchange_lanes(
                        [recv2[pl.ds((h * GZ + t * XL + a) * 8, 8), pl.ds(j * 128, 128)] for a in range(XL)]
                    )
                    for a in range(XL):
                        zz_v[pl.ds((a * J + j) * 8, 8), pl.ds(t * 128, 128)] = tiles[a]

        with jax.named_scope("planes"):
            def border(i, _):
                for k in range(8):
                    x = i * 8 + k
                    zb_v[pl.ds(x, 1), :] = zz_v[pl.ds(x * 8, 1), :]
                    zb_v[pl.ds(XR + x, 1), :] = zz_v[pl.ds(x * 8 + 7, 1), :]
                return 0

            lax.fori_loop(0, XR // 8, border, 0)
            zb_v[pl.ds(2 * XR, 8), :] = zz_v[pl.ds(0, 8), :]
            zb_v[pl.ds(2 * XR + 8, 8), :] = zz_v[pl.ds(ROWS - 8, 8), :]
            part = dot3(split(zb_v[...]), (hh[hrow, :], hl[hrow, :]))
            pb_v[...] = part if h == 0 else pb_v[...] + part

        if h == NH - 1:
            planes = [
                remote(pb_v.at[pl.ds(XR, XR)], zp_v.at[pl.ds(0, XR)], ph_s.at[0], ph_r.at[0], gz(1)),
                remote(pb_v.at[pl.ds(0, XR)], zp_v.at[pl.ds(XR, XR)], ph_s.at[1], ph_r.at[1], gz(GZ - 1)),
                remote(pb_v.at[pl.ds(2 * XR + 8, 8)], px_v.at[pl.ds(0, 8)], ph_s.at[2], ph_r.at[2], xy(1)),
                remote(pb_v.at[pl.ds(2 * XR, 8)], px_v.at[pl.ds(8, 8)], ph_s.at[3], ph_r.at[3], xy(XY - 1)),
            ]

        with jax.named_scope("inverse"):
            def inverse(i, _):
                rows = pl.ds(pl.multiple_of(i * 256, 256), 256)
                out = rows
                part = dot3(split(zz_v[rows, :]), (hh[hrow, :], hl[hrow, :]))
                p_v[out, :] = part if h == 0 else p_v[out, :] + part
                return 0

            lax.fori_loop(0, ROWS // 256, inverse, 0)

    with jax.named_scope("outputs"):
        def outputs(i, _):
            def east(x, p, before):
                return f_v[tile8(x + 1), :] * f_v[tile8(x), :] * (e_v[tile8(x), :] - (p - before))

            p = p_v[tile8(i * 8), :]
            now = east(i * 8, p, p_v[tile8(jnp.maximum(i * 8 - 1, 0)), :])
            for k in range(8):
                x = i * 8 + k
                after = p_v[tile8(jnp.minimum(x + 1, XR - 1) if k == 7 else x + 1), :]
                then = east(x + 1, after, p)
                f = f_v[tile8(x + 1), :]
                north = f * pltpu.roll(f, 1, 1) * (n_v[tile8(x), :] - (p - pltpu.roll(p, 1, 1)))
                up = f * pltpu.roll(f, 1, 0) * (w_v[tile8(x), :] - (p - pltpu.roll(p, 1, 0)))
                up = jnp.where(sub == 0, 0.0, up)
                eo_v[tile8(x), :] = now
                no_v[tile8(x), :] = north
                wo_v[tile8(x), :] = up
                ro_v[tile8(x), :] = (now - then) + (north - pltpu.roll(north, NY - 1, 1)) + (up - pltpu.roll(up, 7, 0))
                now, p = then, after
            return 0

        lax.fori_loop(0, XR // 8, outputs, 0)

    with jax.named_scope("waitend"):
        for h in range(NH):
            wait_bytes(send1.at[pl.ds(h * NZ, NZ - 8)], a_s.at[h])
            wait_bytes(ag_v.at[pl.ds(h * XY * 2 * PR, (XY - 1) * 2 * PR)], g_s.at[h])
            wait_bytes(send2.at[pl.ds(h * NZ, NZ - 8)], b_s.at[h])
        halos[5].wait()
        for c in planes:
            c.wait()
    with jax.named_scope("faces"):
        west = f_v[pl.ds(8, 8), :] * fx_v[pl.ds(0, 8), :]
        west = west * (e_v[pl.ds(0, 8), :] - (p_v[pl.ds(0, 8), :] - px_v[pl.ds(0, 8), :]))
        east = f_v[pl.ds(ROWS, 8), :] * fx_v[pl.ds(8, 8), :]
        east = east * (ex_v[...] - (px_v[pl.ds(8, 8), :] - p_v[pl.ds(ROWS - 8, 8), :]))
        eo_v[pl.ds(0, 8), :] = west
        ro_v[pl.ds(0, 8), :] = ro_v[pl.ds(0, 8), :] + west
        ro_v[pl.ds(ROWS - 8, 8), :] = ro_v[pl.ds(ROWS - 8, 8), :] - east
        below = jnp.where(first, 0.0, zp_v[low, :])
        z0_v[...] = jnp.where(first, 1.0, zf_v[low, :]) * (gs_v[...] - zs_v[high, :] * (pb_v[low, :] - below))
        above = zs_v[low, :] * (ga_v[...] - zf_v[high, :] * (zp_v[high, :] - pb_v[high, :]))
        z7_v[...] = jnp.where(last, 0.0, above)


def last_kernel(p, e, n, w, r, z0, z7, eo, no, wo, po, ro, w_v, r_v, sem):
    copies = [pltpu.make_async_copy(src, dst, sem.at[k]) for k, (src, dst) in enumerate(((e, eo), (n, no), (p, po)))]
    for c in copies:
        c.start()
    sub = lax.broadcasted_iota(jnp.int32, (8, NY), 0)
    for s in range(XR // XS):

        def one(i, _):
            for k in range(8):
                x = s * XS + i * 8 + k
                face = row(z0, x)
                w_v[tile8(x), :] = jnp.where(sub == 0, face, w[tile8(x), :])
                r_v[tile8(x), :] = r[tile8(x), :] + jnp.where(sub == 0, face, jnp.where(sub == 7, -row(z7, x), 0.0))
            return 0

        lax.fori_loop(0, XS // 8, one, 0)
        rows = pl.ds(s * XS * 8, XS * 8)
        for k, (src, dst) in enumerate(((w_v, wo), (r_v, ro))):
            copy = pltpu.make_async_copy(src.at[rows], dst.at[rows], sem.at[3 + 2 * s + k])
            copy.start()
            copies.append(copy)
    for c in copies:
        c.wait()


def tables():
    i = np.arange(NY)
    angle = 2 * np.pi * ((i[:, None] * i[None, :]) % NY) / NY
    hart = np.cos(angle) + np.sin(angle)
    k = np.arange(1, NZ + 1)
    sine = np.sin(np.pi * ((k[:, None] * k[None, :]) % (2 * (NZ + 1))) / (NZ + 1))
    lam = 4 * np.sin(np.pi * i / NY) ** 2
    mu = 4 * np.sin(np.pi * k / (2 * (NZ + 1))) ** 2

    def cut(a):
        hi = a.astype(np.float32).astype(BF16)
        return hi, (a - hi.astype(np.float64)).astype(np.float32).astype(BF16)

    lanes_of = np.arange(128)
    half = np.arange(NH)[:, None, None]
    who = slot(np.arange(GZ))[None, :, None]
    lam = lam[half * LH + who * KL + lanes_of[None, None, :] % KL].reshape(NH * GZ, 128)
    packed = mu[(lanes_of[None, :] // KL) * PR + np.arange(PR)[:, None]]
    mu = np.repeat(mu[:, None], 128, 1)
    return (*cut(hart), *cut(sine), lam.astype(np.float32), mu.astype(np.float32), packed.astype(np.float32))


def local(east_velocity, north_velocity, upward_velocity, obstacle):
    fields = (east_velocity, north_velocity, upward_velocity, obstacle)
    args = [pltpu.with_memory_space_constraint(a.reshape(ROWS, NY), pltpu.HBM) for a in fields]
    args += [pltpu.with_memory_space_constraint(jnp.asarray(t), pltpu.HBM) for t in tables()]
    any_spec = pl.BlockSpec(memory_space=pl.ANY)
    vmem = pl.BlockSpec(memory_space=pltpu.VMEM)

    def v(*shape, dtype=F32):
        return pltpu.VMEM(shape, dtype)

    dma = pltpu.SemaphoreType.DMA
    field = jax.ShapeDtypeStruct((ROWS, NY), F32)
    plane = jax.ShapeDtypeStruct((XR, NY), F32)
    operands = pl.pallas_call(
        main_kernel,
        out_shape=[field] * 5 + [plane] * 2,
        in_specs=[any_spec] * 11,
        out_specs=[vmem] * 7,
        scratch_shapes=[
            v(ROWS + 16, NY), v(ROWS + 8, NY), v(ROWS, NY), v(ROWS, NY), v(2 * XR, NY), v(2 * XR, NY), v(XR, NY), v(16, NY),
            v(ROWS, NY, dtype=jnp.int32), v(ROWS, NY),
            v(NY, NY, dtype=BF16), v(NY, NY, dtype=BF16), v(NZ, NZ, dtype=BF16), v(NZ, NZ, dtype=BF16),
            v(NH * GZ, 128), v(NZ, 128), v(PR, 128),
            v(2 * XR, NY), v(XR, NY), v(16, NY), v(8, NY), v(EDGE, NY), v(NH, EDGE, LH), v(EDGE, LH), v(EDGE, NY),
            v(NH * NZ, 128), v(NH * NZ, 128),
            v(NH * ROWS, LH), v(NH * NZ, W), v(NH * NZ, W), v(NZ, W, dtype=BF16), v(NZ, W, dtype=BF16),
            v(NH * NZ, W), v(NH * NZ, 128), v(NH * NZ, 128), v(NH * NZ, 128), v(NH * NZ, 128),
            v(NH * XY * 2 * PR, 128), v(NH * NZ, W), v(NH * NZ, W), v(ROWS, LH),
            dma((11,)), dma((6,)), dma((6,)), dma((NH,)), dma((NH,)), dma((NH,)), dma((NH,)),
            dma((NH,)), dma((NH,)), dma((4,)), dma((4,)),
        ],
        compiler_params=pltpu.CompilerParams(
            collective_id=0, has_side_effects=True, vmem_limit_bytes=32 * 1024 * 1024
        ),
        name="main",
    )(*args)

    outs = pl.pallas_call(
        last_kernel,
        out_shape=[field] * 5,
        in_specs=[vmem] * 7,
        out_specs=[any_spec] * 5,
        scratch_shapes=[v(ROWS, NY), v(ROWS, NY), dma((3 + 2 * (XR // XS),))],
        compiler_params=pltpu.CompilerParams(vmem_limit_bytes=8 * 1024 * 1024),
        name="last",
    )(*operands)
    return tuple(a.reshape(XR, CZ, NY) for a in outs)


def solution(mesh):
    spec = P("xy", "gz", None)
    return jax.shard_map(local, mesh=mesh, in_specs=(spec,) * 4, out_specs=(spec,) * 5, check_vma=False)
```

```python
import functools

import jax
import jax.numpy as jnp
import numpy as np
from jax import lax
from jax.experimental import pallas as pl
from jax.experimental.pallas import tpu as pltpu
from jax.sharding import PartitionSpec as P

NX = 512
NY = 512
NZ = 256
GZ = 32
XY = 8
XR = NX // XY
CZ = NZ // GZ
NH = 4
KL = NY // GZ // NH
XL = 128 // KL
J = XR // XL
LH = NY // NH
W = J * 128
ROWS = XR * CZ
LOGJ = J.bit_length() - 1
BR = 32
BW = 128
NG = LH // 128
PR = NZ // XL
LAG = 2
XS = 16
EDGE = 2 * XR + 16
F32 = jnp.float32
BF16 = jnp.bfloat16


def split(a):
    hi = a.astype(BF16)
    return hi, (a - hi.astype(F32)).astype(BF16)


def dot(a, b):
    return jnp.dot(a, b, preferred_element_type=F32)


def dot3(a, b):
    return dot(a[0], b[0]) + (dot(a[0], b[1]) + dot(a[1], b[0]))


def lanes(shape):
    return lax.broadcasted_iota(jnp.int32, shape, 1)


def slot(t):
    return t % NG * XL + t // NG


def far_first():
    hops = (0, 1, 2, 1)
    every = [(x, y, c) for x in range(4) for y in range(4) for c in range(2)]
    every.remove((0, 0, 0))
    return sorted(every, key=lambda o: -(hops[o[0]] + hops[o[1]]))


def roll(a, shift):
    return pltpu.roll(a, shift % 128, 1)


def exchange_lanes(tiles):
    tiles = list(tiles)
    group = lanes((8, 128)) // KL
    step = 1
    while step < XL:
        clear = (group & step) == 0
        for i in range(XL):
            if not i & step:
                k = i | step
                a, b = tiles[i], tiles[k]
                tiles[i] = jnp.where(clear, a, roll(b, step * KL))
                tiles[k] = jnp.where(clear, roll(a, -step * KL), b)
        step *= 2
    return tiles


def row(ref, r):
    return jnp.broadcast_to(ref[pl.ds(r, 1), :], (8, ref.shape[1]))


def tile8(at):
    return pl.ds(pl.multiple_of(at * 8, 8), 8)


def main_kernel(
    e_h, n_h, w_h, o_h, hh_h, hl_h, sh_h, sl_h, lam_h, mu_h, mup_h,
    p_v, eo_v, no_v, wo_v, ro_v, z0_v, z7_v,
    f_v, e_v, n_v, w_v, zf_v, ga_v,
    o_v, src_h, src_l, hh, hl, sh, sl, lam, mu, mup,
    zs_v, gs_v, fx_v, ex_v, cc_v, cc_h, cc_l, cy_v, zb_v, zq_v, ph_v, up_v, dn_v,
    y_v, send1, recv1, dh, dl, x_v, ea_v, eb_v, r_v, c_v, ag_v, send2, recv2, zz_v,
    load_sem, halo_s, halo_r, a_s, a_r, g_s, g_r, b_s, b_r, ph_s, ph_r,
):
    me = lax.axis_index("gz")
    xi = lax.axis_index("xy")
    first = me == 0
    last = me == GZ - 1
    spot = lax.rem(me, NG) * XL + me // NG

    def gz(o):
        return {"gz": lax.rem(me + o, GZ)}

    def xy(o):
        return {"xy": lax.rem(xi + o, XY)}

    def peer(o):
        x = lax.rem(me // 8 + o[0], 4)
        y = lax.rem(me // 2 + o[1], 4)
        return (x * 4 + y) * 2 + lax.rem(me + o[2], 2)

    def load(k, src, dst):
        copy = pltpu.make_async_copy(src, dst, load_sem.at[k])
        copy.start()
        return copy

    def remote(src, dst, ssem, rsem, who):
        copy = pltpu.make_async_remote_copy(
            src_ref=src, dst_ref=dst, send_sem=ssem, recv_sem=rsem, device_id=who,
            device_id_type=pl.DeviceIdType.MESH,
        )
        copy.start()
        return copy

    class Shift:
        def __init__(self, src, dst, ssem, rsem, up):
            self.copy = pltpu.make_async_remote_copy(
                src_ref=src, dst_ref=dst, send_sem=ssem, recv_sem=rsem, device_id=gz(1 if up else GZ - 1),
                device_id_type=pl.DeviceIdType.MESH,
            )
            self.sends = me < GZ - 1 if up else me > 0
            self.receives = me > 0 if up else me < GZ - 1
            pl.when(self.sends)(lambda: self.copy.start())

        def wait(self):
            pl.when(self.receives)(lambda: self.copy.wait_recv())
            pl.when(self.sends)(lambda: self.copy.wait_send())

    def wait_bytes(ref, sem):
        pltpu.make_async_copy(ref, ref, sem).wait()

    flags, upward = load(0, o_h, o_v), load(1, w_h, w_v)
    barrier = pltpu.get_barrier_semaphore()

    def greet_gz(o, _):
        pl.semaphore_signal(barrier, inc=1, device_id=gz(o), device_id_type=pl.DeviceIdType.MESH)
        return 0

    def greet_xy(o, _):
        pl.semaphore_signal(barrier, inc=1, device_id=xy(o), device_id_type=pl.DeviceIdType.MESH)
        return 0

    lax.fori_loop(1, XY, greet_xy, 0)
    lax.fori_loop(1, GZ, greet_gz, 0)

    loads = [
        flags,
        upward,
        load(2, e_h, e_v.at[pl.ds(0, ROWS)]),
        load(3, n_h, n_v),
        load(4, hh_h, hh),
        load(5, hl_h, hl),
        load(6, sh_h, sh),
        load(7, sl_h, sl),
        load(8, lam_h, lam),
        load(9, mu_h, mu),
        load(10, mup_h, mup),
    ]

    with jax.named_scope("fluid"):
        loads[0].wait()

        def to_fluid(i, _):
            rows = pl.ds(pl.multiple_of(i * 64, 64), 64)
            f_v[pl.ds(pl.multiple_of(8 + i * 64, 8), 64), :] = (1 - o_v[rows, :]).astype(F32)
            return 0

        lax.fori_loop(0, ROWS // 64, to_fluid, 0)
        f_v[pl.ds(0, 8), :] = jnp.zeros((8, NY), F32)
        f_v[pl.ds(ROWS + 8, 8), :] = jnp.zeros((8, NY), F32)
        e_v[pl.ds(ROWS, 8), :] = jnp.zeros((8, NY), F32)
        loads[1].wait()

        def edge(i, _):
            for k in range(8):
                x = i * 8 + k
                low = f_v[pl.ds(x * 8 + 8, 1), :]
                zs_v[pl.ds(x, 1), :] = f_v[pl.ds(x * 8 + 15, 1), :]
                zs_v[pl.ds(XR + x, 1), :] = low
                gs_v[pl.ds(x, 1), :] = low * w_v[pl.ds(x * 8, 1), :]
            return 0

        lax.fori_loop(0, XR // 8, edge, 0)
    with jax.named_scope("barrier"):
        pl.semaphore_wait(barrier, GZ - 1 + XY - 1)
    halos = [
        Shift(gs_v, ga_v, halo_s.at[0], halo_r.at[0], False),
        Shift(zs_v.at[pl.ds(0, XR)], zf_v.at[pl.ds(0, XR)], halo_s.at[1], halo_r.at[1], True),
        remote(f_v.at[pl.ds(ROWS, 8)], fx_v.at[pl.ds(0, 8)], halo_s.at[2], halo_r.at[2], xy(1)),
        remote(f_v.at[pl.ds(8, 8)], fx_v.at[pl.ds(8, 8)], halo_s.at[3], halo_r.at[3], xy(XY - 1)),
        Shift(zs_v.at[pl.ds(XR, XR)], zf_v.at[pl.ds(XR, XR)], halo_s.at[5], halo_r.at[5], False),
    ]
    @pl.when(first)
    def _():
        zf_v[pl.ds(0, XR), :] = jnp.ones((XR, NY), F32)
        for h in range(NH):
            zq_v[pl.ds(h * EDGE, XR), :] = jnp.zeros((XR, LH), F32)

    @pl.when(last)
    def _():
        ga_v[...] = jnp.zeros((XR, NY), F32)
        zf_v[pl.ds(XR, XR), :] = jnp.zeros((XR, NY), F32)
        for h in range(NH):
            zq_v[pl.ds(h * EDGE + XR, XR), :] = jnp.zeros((XR, LH), F32)

    loads[2].wait()
    halos.append(remote(e_v.at[pl.ds(0, 8)], ex_v, halo_s.at[4], halo_r.at[4], xy(XY - 1)))

    with jax.named_scope("source"):
        loads[3].wait()
        sub = lax.broadcasted_iota(jnp.int32, (8, NY), 0)

        def source(i, _):
            def east(x):
                return f_v[tile8(x + 1), :] * f_v[tile8(x), :] * e_v[tile8(x), :]

            now = east(i * 8)
            pair = []
            for k in range(8):
                x = i * 8 + k
                then = east(x + 1)
                f = f_v[tile8(x + 1), :]
                north = f * pltpu.roll(f, 1, 1) * n_v[tile8(x), :]
                up = jnp.where(sub == 0, 0.0, f * pltpu.roll(f, 1, 0) * w_v[tile8(x), :])
                pair.append((now - then) + (north - pltpu.roll(north, NY - 1, 1)) + (up - pltpu.roll(up, 7, 0)))
                now = then
                if k % 2:
                    rows = pl.ds(pl.multiple_of(i * 64 + (k - 1) * 8, 16), 16)
                    src_h[rows, :], src_l[rows, :] = split(jnp.concatenate(pair, 0))
                    pair = []
            return 0

        lax.fori_loop(0, XR // 8, source, 0)

    with jax.named_scope("forward"):
        for k in range(4, 11):
            loads[k].wait()

        def forward(i, _):
            rows = pl.ds(pl.multiple_of(i * 128, 128), 128)
            y = dot3((src_h[rows, :], src_l[rows, :]), (hh[...], hl[...]))
            for h in range(NH):
                y_v[pl.ds(pl.multiple_of(h * ROWS + i * 128, 128), 128), :] = y[:, h * LH : h * LH + LH]
            return 0

        lax.fori_loop(0, ROWS // 128, forward, 0)

    with jax.named_scope("waithalo"):
        for h in (*halos[:4], halos[5]):
            h.wait()

    with jax.named_scope("edges"):
        low, high = pl.ds(0, XR), pl.ds(XR, XR)
        cc_v[low, :] = zf_v[low, :] * gs_v[...]
        cc_v[high, :] = zs_v[low, :] * ga_v[...] * -1.0
        cc_v[pl.ds(2 * XR, 8), :] = fx_v[pl.ds(0, 8), :] * f_v[pl.ds(8, 8), :] * e_v[pl.ds(0, 8), :]
        cc_v[pl.ds(2 * XR + 8, 8), :] = f_v[pl.ds(ROWS, 8), :] * fx_v[pl.ds(8, 8), :] * ex_v[...] * -1.0
        cc_h[...], cc_l[...] = split(cc_v[...])

    sub1 = lax.broadcasted_iota(jnp.int32, (8, 128), 0)
    for h in range(NH):
        with jax.named_scope("pack"):
            hcol = pl.ds(h * LH, LH)
            cy_v[...] = dot3((cc_h[...], cc_l[...]), (hh[:, hcol], hl[:, hcol]))
            lo, hi = pl.ds(h * ROWS, 8), pl.ds(h * ROWS + ROWS - 8, 8)
            y_v[lo, :] = y_v[lo, :] + cy_v[pl.ds(2 * XR, 8), :]
            y_v[hi, :] = y_v[hi, :] + cy_v[pl.ds(2 * XR + 8, 8), :]
            mine = pl.ds(pl.multiple_of(h * NZ + me * 8, 8), 8)
            for t in range(NG):
                tcol = pl.ds(t * 128, 128)

                for j in range(J):
                    tiles = []
                    for a in range(XL):
                        x = a * J + j
                        below = jnp.broadcast_to(cy_v[pl.ds(x, 1), tcol], (8, 128))
                        above = jnp.broadcast_to(cy_v[pl.ds(XR + x, 1), tcol], (8, 128))
                        extra = jnp.where(sub1 == 0, below, jnp.where(sub1 == 7, above, 0.0))
                        tiles.append(y_v[pl.ds((h * XR + x) * 8, 8), tcol] + extra)
                    tiles = exchange_lanes(tiles)
                    for a in range(XL):
                        send1[pl.ds((h * GZ + t * XL + a) * 8, 8), pl.ds(j * 128, 128)] = tiles[a]

            for o in far_first():
                to = peer(o)
                place = lax.rem(to, NG) * XL + to // NG
                remote(send1.at[tile8(h * GZ + place)], recv1.at[mine], a_s.at[h], a_r.at[h], {"gz": to})
            recv1[mine, :] = send1[tile8(h * GZ + spot), :]

    with jax.named_scope("rates"):
        group_r = lanes((64, 128)) // KL
        for h in range(NH):
            lrow = lam[pl.ds(h * GZ + me, 1), :]

            def rates(i, _):
                rows = pl.ds(pl.multiple_of(i * 64, 64), 64)
                out = pl.ds(pl.multiple_of(h * NZ + i * 64, 64), 64)
                g = mu[rows, :] + lrow
                root = jnp.sqrt(g + 0.25 * g * g)
                r = 1.0 / (1.0 + 0.5 * g + root)
                r_v[out, :] = r
                c_v[out, :] = (1.0 / (NZ + 1) / NY) / root
                pw = r
                for _ in range(LOGJ):
                    pw = pw * pw
                up = jnp.ones_like(r)
                down = jnp.ones_like(r)
                step = 1
                while step < XL:
                    on = (group_r & step) != 0
                    up = jnp.where(on, up * pw, up)
                    down = jnp.where(on, down, down * pw)
                    pw = pw * pw
                    step *= 2
                up_v[out, :] = up
                dn_v[out, :] = down
                return 0

            lax.fori_loop(0, NZ // 64, rates, 0)

    group = lanes((PR, 128)) // KL
    wide = lanes((BW, 128)) // KL
    home = lax.broadcasted_iota(jnp.int32, (BW, 128), 0) // PR - wide
    QS = BW // PR

    def descend(h):
        with jax.named_scope("waita2a"):
            wait_bytes(recv1.at[pl.ds(h * NZ, NZ - 8)], a_r.at[h])

        with jax.named_scope("dst"):
            def cut(i, _):
                rows = pl.ds(pl.multiple_of(i * 32, 32), 32)
                a, b = split(recv1[pl.ds(pl.multiple_of(h * NZ + i * 32, 32), 32), :])
                dh[rows, :] = a
                dl[rows, :] = b
                return 0

            lax.fori_loop(0, NZ // 32, cut, 0)
            for c in range(W // 256):
                col = pl.ds(c * 256, 256)
                x_v[pl.ds(h * NZ, NZ), col] = dot3((sh[...], sl[...]), (dh[:, col], dl[:, col]))

        with jax.named_scope("sums"):
            def sums(i, _):
                rows = pl.ds(pl.multiple_of(h * NZ + i * BR, BR), BR)
                r = r_v[rows, :]
                s = [x_v[rows, pl.ds(j * 128, 128)] for j in range(J)]
                u = [s[0]]
                for j in range(1, J):
                    u.append(s[j] + r * u[-1])
                v = [s[-1]]
                for j in range(J - 2, -1, -1):
                    v.append(s[j] + r * v[-1])
                v = v[::-1]
                for j in range(J):
                    x_v[rows, pl.ds(j * 128, 128)] = u[j] + v[j] - s[j]
                ea_v[rows, :] = u[-1]
                eb_v[rows, :] = v[0]
                return 0

            lax.fori_loop(0, NZ // BR, sums, 0)
            pa = jnp.zeros((PR, 128), F32)
            pb = jnp.zeros((PR, 128), F32)
            for i in range(NZ // BW):
                rows = pl.ds(h * NZ + i * BW, BW)
                a, b = ea_v[rows, :], eb_v[rows, :]
                pw = r_v[rows, :]
                for _ in range(LOGJ):
                    pw = pw * pw
                step = 1
                while step < XL:
                    a = a + jnp.where(wide >= step, pw * roll(a, step * KL), 0.0)
                    b = b + jnp.where(wide < XL - step, pw * roll(b, -step * KL), 0.0)
                    pw = pw * pw
                    step *= 2
                ea_v[rows, :] = jnp.where(wide >= 1, roll(a, KL), 0.0)
                eb_v[rows, :] = jnp.where(wide < XL - 1, roll(b, -KL), 0.0)
                for k in range(QS):
                    q = i * QS + k
                    piece = slice(k * PR, k * PR + PR)
                    pa = jnp.where(group == q, roll(a[piece], (q + 1) * KL), pa)
                    pb = jnp.where(group == q, roll(b[piece], q * KL), pb)

        with jax.named_scope("gather"):
            at = pl.multiple_of((h * XY + xi) * 2 * PR, 2 * PR)
            own = pl.ds(at, 2 * PR)
            ag_v[pl.ds(at, PR), :] = pa
            ag_v[pl.ds(pl.multiple_of(at + PR, PR), PR), :] = pb

            def spread(o, _):
                remote(ag_v.at[own], ag_v.at[own], g_s.at[h], g_r.at[h], xy(o))
                return 0

            lax.fori_loop(1, XY, spread, 0)

    def ascend(h):
        with jax.named_scope("waitgather"):
            wait_bytes(ag_v.at[pl.ds(h * XY * 2 * PR, (XY - 1) * 2 * PR)], g_r.at[h])
        with jax.named_scope("finish"):
            g = mup[...] + lam[pl.ds(h * GZ + me, 1), :]
            rp = 1.0 / (1.0 + 0.5 * g + jnp.sqrt(g + 0.25 * g * g))
            for _ in range(XR.bit_length() - 1):
                rp = rp * rp
            full = rp
            for _ in range(XY.bit_length() - 1):
                full = full * full
            close = 1.0 / (1.0 - full)

            def piece(o, part):
                at = (h * XY + lax.rem(xi + o, XY)) * 2 * PR + part * PR
                return ag_v[pl.ds(pl.multiple_of(at, PR), PR), :]

            un, vn = piece(0, 0), piece(0, 1)
            for o in range(1, XY):
                un = un * rp + piece(o, 0)
                vn = vn * rp + piece(XY - o, 1)
            un = un * close
            vn = vn * close

            for i in range(NZ // BW):
                rows = pl.ds(h * NZ + i * BW, BW)
                at = home == -(i * QS)
                ub = jnp.where(at, jnp.concatenate([un] * QS, 0), 0.0)
                vb = jnp.where(at, jnp.concatenate([vn] * QS, 0), 0.0)
                step = 1
                while step < XL:
                    ub = ub + roll(ub, step * KL)
                    vb = vb + roll(vb, step * KL)
                    step *= 2
                ea_v[rows, :] = ea_v[rows, :] + up_v[rows, :] * ub
                eb_v[rows, :] = eb_v[rows, :] + dn_v[rows, :] * vb

            def finish(i, _):
                rows = pl.ds(pl.multiple_of(h * NZ + i * BR, BR), BR)
                out = pl.ds(pl.multiple_of(i * BR, BR), BR)
                r = r_v[rows, :]
                c = c_v[rows, :]
                cu = [r * ea_v[rows, :]]
                cv = [r * eb_v[rows, :]]
                for _ in range(J - 1):
                    cu.append(r * cu[-1])
                    cv.append(r * cv[-1])
                for j in range(J):
                    col = pl.ds(j * 128, 128)
                    a, b = split(c * (x_v[rows, col] + cu[j] + cv[J - 1 - j]))
                    dh[out, col] = a
                    dl[out, col] = b
                return 0

            lax.fori_loop(0, NZ // BR, finish, 0)

        with jax.named_scope("idst"):
            for c in range(W // 256):
                col = pl.ds(c * 256, 256)
                send2[pl.ds(h * NZ, NZ), col] = dot3((sh[...], sl[...]), (dh[:, col], dl[:, col]))

        with jax.named_scope("back"):
            mine = tile8(h * GZ + spot)

            for o in far_first():
                to = peer(o)
                remote(send2.at[tile8(h * GZ + to)], recv2.at[mine], b_s.at[h], b_r.at[h], {"gz": to})
            recv2[mine, :] = send2[tile8(h * GZ + me), :]

    for k in range(NH + LAG):
        if k < NH:
            descend(k)
        if k >= LAG:
            ascend(k - LAG)

    def neighbours():
        total = None
        for h in range(NH):
            for c in planes[h]:
                c.wait()
            rows, hrow = pl.ds(h * EDGE, EDGE), pl.ds(h * LH, LH)
            part = dot3(split(zb_v[rows, :] - zq_v[rows, :]), (hh[hrow, :], hl[hrow, :]))
            total = part if h == 0 else total + part
        ph_v[...] = total

    planes = []
    for h in range(NH):
        hrow = pl.ds(h * LH, LH)
        with jax.named_scope("waitback"):
            wait_bytes(recv2.at[pl.ds(h * NZ, NZ - 8)], b_r.at[h])

        with jax.named_scope("unpack"):
            for t in range(NG):
                for j in range(J):
                    tiles = exchange_lanes(
                        [recv2[pl.ds((h * GZ + t * XL + a) * 8, 8), pl.ds(j * 128, 128)] for a in range(XL)]
                    )
                    for a in range(XL):
                        zz_v[pl.ds((a * J + j) * 8, 8), pl.ds(t * 128, 128)] = tiles[a]

        with jax.named_scope("planes"):
            edge0 = h * EDGE

            def border(i, _):
                for k in range(8):
                    x = i * 8 + k
                    zb_v[pl.ds(edge0 + x, 1), :] = zz_v[pl.ds(x * 8, 1), :]
                    zb_v[pl.ds(edge0 + XR + x, 1), :] = zz_v[pl.ds(x * 8 + 7, 1), :]
                return 0

            lax.fori_loop(0, XR // 8, border, 0)
            zb_v[pl.ds(edge0 + 2 * XR, 8), :] = zz_v[pl.ds(0, 8), :]
            zb_v[pl.ds(edge0 + 2 * XR + 8, 8), :] = zz_v[pl.ds(ROWS - 8, 8), :]
            routes = (
                (XR, 0, XR, True),
                (0, XR, XR, False),
                (2 * XR + 8, 2 * XR, 8, xy(1)),
                (2 * XR, 2 * XR + 8, 8, xy(XY - 1)),
            )
            planes.append([
                (Shift if k < 2 else remote)(
                    zb_v.at[pl.ds(edge0 + a, size)], zq_v.at[pl.ds(edge0 + b, size)],
                    ph_s.at[4 * h + k], ph_r.at[4 * h + k], who,
                )
                for k, (a, b, size, who) in enumerate(routes)
            ])

        with jax.named_scope("inverse"):
            def inverse(i, _):
                rows = pl.ds(pl.multiple_of(i * 256, 256), 256)
                out = rows
                part = dot3(split(zz_v[rows, :]), (hh[hrow, :], hl[hrow, :]))
                p_v[out, :] = part if h == 0 else p_v[out, :] + part
                return 0

            lax.fori_loop(0, ROWS // 256, inverse, 0)

    with jax.named_scope("outputs"):

        def outputs(i, _):
            def east(x, p, before):
                return f_v[tile8(x + 1), :] * f_v[tile8(x), :] * (e_v[tile8(x), :] - (p - before))

            p = p_v[tile8(i * 8), :]
            now = east(i * 8, p, p_v[tile8(jnp.maximum(i * 8 - 1, 0)), :])
            for k in range(8):
                x = i * 8 + k
                after = p_v[tile8(jnp.minimum(x + 1, XR - 1) if k == 7 else x + 1), :]
                then = east(x + 1, after, p)
                f = f_v[tile8(x + 1), :]
                north = f * pltpu.roll(f, 1, 1) * (n_v[tile8(x), :] - (p - pltpu.roll(p, 1, 1)))
                up = f * pltpu.roll(f, 1, 0) * (w_v[tile8(x), :] - (p - pltpu.roll(p, 1, 0)))
                up = jnp.where(sub == 0, 0.0, up)
                eo_v[tile8(x), :] = now
                no_v[tile8(x), :] = north
                wo_v[tile8(x), :] = up
                ro_v[tile8(x), :] = (now - then) + (north - pltpu.roll(north, NY - 1, 1)) + (up - pltpu.roll(up, 7, 0))
                now, p = then, after
            return 0

        lax.fori_loop(0, XR // 8, outputs, 0)

    with jax.named_scope("waitend"):
        for h in range(NH):
            wait_bytes(send1.at[pl.ds(h * NZ, NZ - 8)], a_s.at[h])
            wait_bytes(ag_v.at[pl.ds(h * XY * 2 * PR, (XY - 1) * 2 * PR)], g_s.at[h])
            wait_bytes(send2.at[pl.ds(h * NZ, NZ - 8)], b_s.at[h])
        halos[4].wait()
        neighbours()
    with jax.named_scope("faces"):
        west = f_v[pl.ds(8, 8), :] * fx_v[pl.ds(0, 8), :]
        west = west * (e_v[pl.ds(0, 8), :] - ph_v[pl.ds(2 * XR, 8), :])
        east = f_v[pl.ds(ROWS, 8), :] * fx_v[pl.ds(8, 8), :]
        east = east * (ex_v[...] + ph_v[pl.ds(2 * XR + 8, 8), :])
        eo_v[pl.ds(0, 8), :] = west
        ro_v[pl.ds(0, 8), :] = ro_v[pl.ds(0, 8), :] + west
        ro_v[pl.ds(ROWS - 8, 8), :] = ro_v[pl.ds(ROWS - 8, 8), :] - east
        z0_v[...] = zf_v[low, :] * (gs_v[...] - zs_v[high, :] * ph_v[low, :])
        z7_v[...] = zs_v[low, :] * (ga_v[...] + zf_v[high, :] * ph_v[high, :])


def last_kernel(p, e, n, w, r, z0, z7, eo, no, wo, po, ro, w_v, r_v, sem):
    copies = []

    def out(src, dst, part):
        rows = pl.ds(part * XS * 8, XS * 8)
        copies.append(pltpu.make_async_copy(src.at[rows], dst.at[rows], sem.at[len(copies)]))
        copies[-1].start()

    for src, dst in ((e, eo), (n, no), (p, po)):
        for part in range(XR // XS):
            out(src, dst, part)
    sub = lax.broadcasted_iota(jnp.int32, (8, NY), 0)
    for s in range(XR // XS):

        def one(i, _):
            for k in range(8):
                x = s * XS + i * 8 + k
                face = row(z0, x)
                w_v[tile8(x), :] = jnp.where(sub == 0, face, w[tile8(x), :])
                r_v[tile8(x), :] = r[tile8(x), :] + jnp.where(sub == 0, face, jnp.where(sub == 7, -row(z7, x), 0.0))
            return 0

        lax.fori_loop(0, XS // 8, one, 0)
        out(w_v, wo, s)
        out(r_v, ro, s)
    for c in copies:
        c.wait()


def tables():
    i = np.arange(NY)
    angle = 2 * np.pi * ((i[:, None] * i[None, :]) % NY) / NY
    hart = np.cos(angle) + np.sin(angle)
    k = np.arange(1, NZ + 1)
    sine = np.sin(np.pi * ((k[:, None] * k[None, :]) % (2 * (NZ + 1))) / (NZ + 1))
    lam = 4 * np.sin(np.pi * i / NY) ** 2
    mu = 4 * np.sin(np.pi * k / (2 * (NZ + 1))) ** 2

    def cut(a):
        hi = a.astype(np.float32).astype(BF16)
        return hi, (a - hi.astype(np.float64)).astype(np.float32).astype(BF16)

    lanes_of = np.arange(128)
    half = np.arange(NH)[:, None, None]
    who = slot(np.arange(GZ))[None, :, None]
    lam = lam[half * LH + who * KL + lanes_of[None, None, :] % KL].reshape(NH * GZ, 128)
    packed = mu[(lanes_of[None, :] // KL) * PR + np.arange(PR)[:, None]]
    mu = np.repeat(mu[:, None], 128, 1)
    return (*cut(hart), *cut(sine), lam.astype(np.float32), mu.astype(np.float32), packed.astype(np.float32))


def local(east_velocity, north_velocity, upward_velocity, obstacle):
    fields = (east_velocity, north_velocity, upward_velocity, obstacle)
    args = [pltpu.with_memory_space_constraint(a.reshape(ROWS, NY), pltpu.HBM) for a in fields]
    args += [pltpu.with_memory_space_constraint(jnp.asarray(t), pltpu.HBM) for t in tables()]
    any_spec = pl.BlockSpec(memory_space=pl.ANY)
    vmem = pl.BlockSpec(memory_space=pltpu.VMEM)

    def v(*shape, dtype=F32):
        return pltpu.VMEM(shape, dtype)

    dma = pltpu.SemaphoreType.DMA
    field = jax.ShapeDtypeStruct((ROWS, NY), F32)
    plane = jax.ShapeDtypeStruct((XR, NY), F32)
    operands = pl.pallas_call(
        main_kernel,
        out_shape=[field] * 5 + [plane] * 2,
        in_specs=[any_spec] * 11,
        out_specs=[vmem] * 7,
        scratch_shapes=[
            v(ROWS + 16, NY), v(ROWS + 8, NY), v(ROWS, NY), v(ROWS, NY), v(2 * XR, NY), v(XR, NY),
            v(ROWS, NY, dtype=jnp.int32), v(ROWS, NY, dtype=BF16), v(ROWS, NY, dtype=BF16),
            v(NY, NY, dtype=BF16), v(NY, NY, dtype=BF16), v(NZ, NZ, dtype=BF16), v(NZ, NZ, dtype=BF16),
            v(NH * GZ, 128), v(NZ, 128), v(PR, 128),
            v(2 * XR, NY), v(XR, NY), v(16, NY), v(8, NY), v(EDGE, NY), v(EDGE, NY, dtype=BF16), v(EDGE, NY, dtype=BF16), v(EDGE, LH), v(NH * EDGE, LH), v(NH * EDGE, LH), v(EDGE, NY),
            v(NH * NZ, 128), v(NH * NZ, 128),
            v(NH * ROWS, LH), v(NH * NZ, W), v(NH * NZ, W), v(NZ, W, dtype=BF16), v(NZ, W, dtype=BF16),
            v(NH * NZ, W), v(NH * NZ, 128), v(NH * NZ, 128), v(NH * NZ, 128), v(NH * NZ, 128),
            v(NH * XY * 2 * PR, 128), v(NH * NZ, W), v(NH * NZ, W), v(ROWS, LH),
            dma((11,)), dma((6,)), dma((6,)), dma((NH,)), dma((NH,)), dma((NH,)), dma((NH,)),
            dma((NH,)), dma((NH,)), dma((4 * NH,)), dma((4 * NH,)),
        ],
        compiler_params=pltpu.CompilerParams(
            collective_id=0, has_side_effects=True, vmem_limit_bytes=32 * 1024 * 1024
        ),
        name="main",
    )(*args)

    outs = pl.pallas_call(
        last_kernel,
        out_shape=[field] * 5,
        in_specs=[vmem] * 7,
        out_specs=[any_spec] * 5,
        scratch_shapes=[v(ROWS, NY), v(ROWS, NY), dma((5 * (XR // XS),))],
        compiler_params=pltpu.CompilerParams(vmem_limit_bytes=8 * 1024 * 1024),
        name="last",
    )(*operands)
    return tuple(a.reshape(XR, CZ, NY) for a in outs)


def solution(mesh):
    spec = P("xy", "gz", None)
    return jax.shard_map(local, mesh=mesh, in_specs=(spec,) * 4, out_specs=(spec,) * 5, check_vma=False)
```

```python
import functools

import jax
import jax.numpy as jnp
import numpy as np
from jax import lax
from jax.experimental import pallas as pl
from jax.experimental.pallas import tpu as pltpu
from jax.sharding import PartitionSpec as P

NX = 512
NY = 512
NZ = 256
GZ = 32
XY = 8
XR = NX // XY
CZ = NZ // GZ
NH = 4
KL = NY // GZ // NH
XL = 128 // KL
J = XR // XL
LH = NY // NH
W = J * 128
ROWS = XR * CZ
LOGJ = J.bit_length() - 1
BR = 32
BW = 256
NG = LH // 128
PR = NZ // XL
LAG = 2
XS = 16
EDGE = 2 * XR + 16
F32 = jnp.float32
BF16 = jnp.bfloat16


def split(a):
    hi = a.astype(BF16)
    return hi, (a - hi.astype(F32)).astype(BF16)


def dot(a, b):
    return jnp.dot(a, b, preferred_element_type=F32)


def dot3(a, b):
    return dot(a[0], b[0]) + (dot(a[0], b[1]) + dot(a[1], b[0]))


def lanes(shape):
    return lax.broadcasted_iota(jnp.int32, shape, 1)


def slot(t):
    return t % NG * XL + t // NG


def far_first():
    hops = (0, 1, 2, 1)
    every = [(x, y, c) for x in range(4) for y in range(4) for c in range(2)]
    every.remove((0, 0, 0))
    return sorted(every, key=lambda o: -(hops[o[0]] + hops[o[1]]))


def roll(a, shift):
    return pltpu.roll(a, shift % 128, 1)


def exchange_lanes(tiles):
    tiles = list(tiles)
    group = lanes((8, 128)) // KL
    step = 1
    while step < XL:
        clear = (group & step) == 0
        for i in range(XL):
            if not i & step:
                k = i | step
                a, b = tiles[i], tiles[k]
                tiles[i] = jnp.where(clear, a, roll(b, step * KL))
                tiles[k] = jnp.where(clear, roll(a, -step * KL), b)
        step *= 2
    return tiles


def row(ref, r):
    return jnp.broadcast_to(ref[pl.ds(r, 1), :], (8, ref.shape[1]))


def tile8(at):
    return pl.ds(pl.multiple_of(at * 8, 8), 8)


def main_kernel(
    e_h, n_h, w_h, o_h, hh_h, hl_h, sh_h, sl_h, lam_h, mu_h, mup_h,
    p_v, eo_v, no_v, wo_v, ro_v, z0_v, z7_v,
    f_v, e_v, n_v, w_v, zf_v, ga_v,
    o_v, src_h, src_l, hh, hl, sh, sl, lam, mu, mup,
    zs_v, gs_v, fx_v, ex_v, cc_v, cc_h, cc_l, cy_v, zb_v, zq_v, ph_v, up_v, dn_v,
    y_v, send1, recv1, dh, dl, x_v, ea_v, eb_v, r_v, c_v, ag_v, send2, recv2, zz_v,
    load_sem, halo_s, halo_r, a_s, a_r, g_s, g_r, b_s, b_r, ph_s, ph_r,
):
    me = lax.axis_index("gz")
    xi = lax.axis_index("xy")
    first = me == 0
    last = me == GZ - 1
    spot = lax.rem(me, NG) * XL + me // NG

    def gz(o):
        return {"gz": lax.rem(me + o, GZ)}

    def xy(o):
        return {"xy": lax.rem(xi + o, XY)}

    def peer(o):
        x = lax.rem(me // 8 + o[0], 4)
        y = lax.rem(me // 2 + o[1], 4)
        return (x * 4 + y) * 2 + lax.rem(me + o[2], 2)

    def load(k, src, dst):
        copy = pltpu.make_async_copy(src, dst, load_sem.at[k])
        copy.start()
        return copy

    def remote(src, dst, ssem, rsem, who):
        copy = pltpu.make_async_remote_copy(
            src_ref=src, dst_ref=dst, send_sem=ssem, recv_sem=rsem, device_id=who,
            device_id_type=pl.DeviceIdType.MESH,
        )
        copy.start()
        return copy

    class Shift:
        def __init__(self, src, dst, ssem, rsem, up):
            self.copy = pltpu.make_async_remote_copy(
                src_ref=src, dst_ref=dst, send_sem=ssem, recv_sem=rsem, device_id=gz(1 if up else GZ - 1),
                device_id_type=pl.DeviceIdType.MESH,
            )
            self.sends = me < GZ - 1 if up else me > 0
            self.receives = me > 0 if up else me < GZ - 1
            pl.when(self.sends)(lambda: self.copy.start())

        def wait(self):
            pl.when(self.receives)(lambda: self.copy.wait_recv())
            pl.when(self.sends)(lambda: self.copy.wait_send())

    def wait_bytes(ref, sem):
        pltpu.make_async_copy(ref, ref, sem).wait()

    flags, upward = load(0, o_h, o_v), load(1, w_h, w_v)
    barrier = pltpu.get_barrier_semaphore()

    def greet_gz(o, _):
        pl.semaphore_signal(barrier, inc=1, device_id=gz(o), device_id_type=pl.DeviceIdType.MESH)
        return 0

    def greet_xy(o, _):
        pl.semaphore_signal(barrier, inc=1, device_id=xy(o), device_id_type=pl.DeviceIdType.MESH)
        return 0

    lax.fori_loop(1, XY, greet_xy, 0)
    lax.fori_loop(1, GZ, greet_gz, 0)

    loads = [
        flags,
        upward,
        load(2, e_h, e_v.at[pl.ds(0, ROWS)]),
        load(3, n_h, n_v),
        load(4, hh_h, hh),
        load(5, hl_h, hl),
        load(6, sh_h, sh),
        load(7, sl_h, sl),
        load(8, lam_h, lam),
        load(9, mu_h, mu),
        load(10, mup_h, mup),
    ]

    with jax.named_scope("fluid"):
        loads[0].wait()

        def to_fluid(i, _):
            rows = pl.ds(pl.multiple_of(i * 64, 64), 64)
            f_v[pl.ds(pl.multiple_of(8 + i * 64, 8), 64), :] = (1 - o_v[rows, :]).astype(F32)
            return 0

        lax.fori_loop(0, ROWS // 64, to_fluid, 0)
        f_v[pl.ds(0, 8), :] = jnp.zeros((8, NY), F32)
        f_v[pl.ds(ROWS + 8, 8), :] = jnp.zeros((8, NY), F32)
        e_v[pl.ds(ROWS, 8), :] = jnp.zeros((8, NY), F32)
        loads[1].wait()

        def edge(i, _):
            for k in range(8):
                x = i * 8 + k
                low = f_v[pl.ds(x * 8 + 8, 1), :]
                zs_v[pl.ds(x, 1), :] = f_v[pl.ds(x * 8 + 15, 1), :]
                zs_v[pl.ds(XR + x, 1), :] = low
                gs_v[pl.ds(x, 1), :] = low * w_v[pl.ds(x * 8, 1), :]
            return 0

        lax.fori_loop(0, XR // 8, edge, 0)
    with jax.named_scope("barrier"):
        pl.semaphore_wait(barrier, GZ - 1 + XY - 1)
    halos = [
        Shift(gs_v, ga_v, halo_s.at[0], halo_r.at[0], False),
        Shift(zs_v.at[pl.ds(0, XR)], zf_v.at[pl.ds(0, XR)], halo_s.at[1], halo_r.at[1], True),
        remote(f_v.at[pl.ds(ROWS, 8)], fx_v.at[pl.ds(0, 8)], halo_s.at[2], halo_r.at[2], xy(1)),
        remote(f_v.at[pl.ds(8, 8)], fx_v.at[pl.ds(8, 8)], halo_s.at[3], halo_r.at[3], xy(XY - 1)),
        Shift(zs_v.at[pl.ds(XR, XR)], zf_v.at[pl.ds(XR, XR)], halo_s.at[5], halo_r.at[5], False),
    ]
    @pl.when(first)
    def _():
        zf_v[pl.ds(0, XR), :] = jnp.ones((XR, NY), F32)
        for h in range(NH):
            zq_v[pl.ds(h * EDGE, XR), :] = jnp.zeros((XR, LH), F32)

    @pl.when(last)
    def _():
        ga_v[...] = jnp.zeros((XR, NY), F32)
        zf_v[pl.ds(XR, XR), :] = jnp.zeros((XR, NY), F32)
        for h in range(NH):
            zq_v[pl.ds(h * EDGE + XR, XR), :] = jnp.zeros((XR, LH), F32)

    loads[2].wait()
    halos.append(remote(e_v.at[pl.ds(0, 8)], ex_v, halo_s.at[4], halo_r.at[4], xy(XY - 1)))

    with jax.named_scope("source"):
        loads[3].wait()
        sub = lax.broadcasted_iota(jnp.int32, (8, NY), 0)

        def source(i, _):
            def east(x):
                return f_v[tile8(x + 1), :] * f_v[tile8(x), :] * e_v[tile8(x), :]

            now = east(i * 8)
            pair = []
            for k in range(8):
                x = i * 8 + k
                then = east(x + 1)
                f = f_v[tile8(x + 1), :]
                north = f * pltpu.roll(f, 1, 1) * n_v[tile8(x), :]
                up = jnp.where(sub == 0, 0.0, f * pltpu.roll(f, 1, 0) * w_v[tile8(x), :])
                pair.append((now - then) + (north - pltpu.roll(north, NY - 1, 1)) + (up - pltpu.roll(up, 7, 0)))
                now = then
                if k % 2:
                    rows = pl.ds(pl.multiple_of(i * 64 + (k - 1) * 8, 16), 16)
                    src_h[rows, :], src_l[rows, :] = split(jnp.concatenate(pair, 0))
                    pair = []
            return 0

        lax.fori_loop(0, XR // 8, source, 0)

    with jax.named_scope("forward"):
        for k in range(4, 11):
            loads[k].wait()

        def forward(i, _):
            rows = pl.ds(pl.multiple_of(i * 128, 128), 128)
            y = dot3((src_h[rows, :], src_l[rows, :]), (hh[...], hl[...]))
            for h in range(NH):
                y_v[pl.ds(pl.multiple_of(h * ROWS + i * 128, 128), 128), :] = y[:, h * LH : h * LH + LH]
            return 0

        lax.fori_loop(0, ROWS // 128, forward, 0)

    with jax.named_scope("waithalo"):
        for h in (*halos[:4], halos[5]):
            h.wait()

    with jax.named_scope("edges"):
        low, high = pl.ds(0, XR), pl.ds(XR, XR)
        cc_v[low, :] = zf_v[low, :] * gs_v[...]
        cc_v[high, :] = zs_v[low, :] * ga_v[...] * -1.0
        cc_v[pl.ds(2 * XR, 8), :] = fx_v[pl.ds(0, 8), :] * f_v[pl.ds(8, 8), :] * e_v[pl.ds(0, 8), :]
        cc_v[pl.ds(2 * XR + 8, 8), :] = f_v[pl.ds(ROWS, 8), :] * fx_v[pl.ds(8, 8), :] * ex_v[...] * -1.0
        cc_h[...], cc_l[...] = split(cc_v[...])

    sub1 = lax.broadcasted_iota(jnp.int32, (8, 128), 0)
    for h in range(NH):
        with jax.named_scope("pack"):
            hcol = pl.ds(h * LH, LH)
            cy_v[...] = dot3((cc_h[...], cc_l[...]), (hh[:, hcol], hl[:, hcol]))
            lo, hi = pl.ds(h * ROWS, 8), pl.ds(h * ROWS + ROWS - 8, 8)
            y_v[lo, :] = y_v[lo, :] + cy_v[pl.ds(2 * XR, 8), :]
            y_v[hi, :] = y_v[hi, :] + cy_v[pl.ds(2 * XR + 8, 8), :]
            mine = pl.ds(pl.multiple_of(h * NZ + me * 8, 8), 8)
            for t in range(NG):
                tcol = pl.ds(t * 128, 128)

                for j in range(J):
                    tiles = []
                    for a in range(XL):
                        x = a * J + j
                        below = jnp.broadcast_to(cy_v[pl.ds(x, 1), tcol], (8, 128))
                        above = jnp.broadcast_to(cy_v[pl.ds(XR + x, 1), tcol], (8, 128))
                        extra = jnp.where(sub1 == 0, below, jnp.where(sub1 == 7, above, 0.0))
                        tiles.append(y_v[pl.ds((h * XR + x) * 8, 8), tcol] + extra)
                    tiles = exchange_lanes(tiles)
                    for a in range(XL):
                        send1[pl.ds((h * GZ + t * XL + a) * 8, 8), pl.ds(j * 128, 128)] = tiles[a]

            for o in far_first():
                to = peer(o)
                place = lax.rem(to, NG) * XL + to // NG
                remote(send1.at[tile8(h * GZ + place)], recv1.at[mine], a_s.at[h], a_r.at[h], {"gz": to})
            recv1[mine, :] = send1[tile8(h * GZ + spot), :]

    with jax.named_scope("rates"):
        group_r = lanes((64, 128)) // KL
        for h in range(NH):
            lrow = lam[pl.ds(h * GZ + me, 1), :]

            def rates(i, _):
                rows = pl.ds(pl.multiple_of(i * 64, 64), 64)
                out = pl.ds(pl.multiple_of(h * NZ + i * 64, 64), 64)
                g = mu[rows, :] + lrow
                root = jnp.sqrt(g + 0.25 * g * g)
                r = 1.0 / (1.0 + 0.5 * g + root)
                r_v[out, :] = r
                c_v[out, :] = (1.0 / (NZ + 1) / NY) / root
                pw = r
                for _ in range(LOGJ):
                    pw = pw * pw
                up = jnp.ones_like(r)
                down = jnp.ones_like(r)
                step = 1
                while step < XL:
                    on = (group_r & step) != 0
                    up = jnp.where(on, up * pw, up)
                    down = jnp.where(on, down, down * pw)
                    pw = pw * pw
                    step *= 2
                up_v[out, :] = up
                dn_v[out, :] = down
                return 0

            lax.fori_loop(0, NZ // 64, rates, 0)

    group = lanes((PR, 128)) // KL
    wide = lanes((BW, 128)) // KL
    home = lax.broadcasted_iota(jnp.int32, (BW, 128), 0) // PR - wide
    QS = BW // PR

    def descend(h):
        with jax.named_scope("waita2a"):
            wait_bytes(recv1.at[pl.ds(h * NZ, NZ - 8)], a_r.at[h])

        with jax.named_scope("dst"):
            def cut(i, _):
                rows = pl.ds(pl.multiple_of(i * 32, 32), 32)
                a, b = split(recv1[pl.ds(pl.multiple_of(h * NZ + i * 32, 32), 32), :])
                dh[rows, :] = a
                dl[rows, :] = b
                return 0

            lax.fori_loop(0, NZ // 32, cut, 0)
            for c in range(W // 256):
                col = pl.ds(c * 256, 256)
                x_v[pl.ds(h * NZ, NZ), col] = dot3((sh[...], sl[...]), (dh[:, col], dl[:, col]))

        with jax.named_scope("sums"):
            def sums(i, _):
                rows = pl.ds(pl.multiple_of(h * NZ + i * BR, BR), BR)
                r = r_v[rows, :]
                s = [x_v[rows, pl.ds(j * 128, 128)] for j in range(J)]
                u = [s[0]]
                for j in range(1, J):
                    u.append(s[j] + r * u[-1])
                v = [s[-1]]
                for j in range(J - 2, -1, -1):
                    v.append(s[j] + r * v[-1])
                v = v[::-1]
                for j in range(J):
                    x_v[rows, pl.ds(j * 128, 128)] = u[j] + v[j] - s[j]
                ea_v[rows, :] = u[-1]
                eb_v[rows, :] = v[0]
                return 0

            lax.fori_loop(0, NZ // BR, sums, 0)
            pa = jnp.zeros((PR, 128), F32)
            pb = jnp.zeros((PR, 128), F32)
            for i in range(NZ // BW):
                rows = pl.ds(h * NZ + i * BW, BW)
                a, b = ea_v[rows, :], eb_v[rows, :]
                pw = r_v[rows, :]
                for _ in range(LOGJ):
                    pw = pw * pw
                step = 1
                while step < XL:
                    a = a + jnp.where(wide >= step, pw * roll(a, step * KL), 0.0)
                    b = b + jnp.where(wide < XL - step, pw * roll(b, -step * KL), 0.0)
                    pw = pw * pw
                    step *= 2
                ea_v[rows, :] = jnp.where(wide >= 1, roll(a, KL), 0.0)
                eb_v[rows, :] = jnp.where(wide < XL - 1, roll(b, -KL), 0.0)
                for k in range(QS):
                    q = i * QS + k
                    piece = slice(k * PR, k * PR + PR)
                    pa = jnp.where(group == q, roll(a[piece], (q + 1) * KL), pa)
                    pb = jnp.where(group == q, roll(b[piece], q * KL), pb)

        with jax.named_scope("gather"):
            at = pl.multiple_of((h * XY + xi) * 2 * PR, 2 * PR)
            own = pl.ds(at, 2 * PR)
            ag_v[pl.ds(at, PR), :] = pa
            ag_v[pl.ds(pl.multiple_of(at + PR, PR), PR), :] = pb

            for o in sorted(range(1, XY), key=lambda o: -min(o, XY - o)):
                remote(ag_v.at[own], ag_v.at[own], g_s.at[h], g_r.at[h], xy(o))

    def ascend(h):
        with jax.named_scope("waitgather"):
            wait_bytes(ag_v.at[pl.ds(h * XY * 2 * PR, (XY - 1) * 2 * PR)], g_r.at[h])
        with jax.named_scope("finish"):
            g = mup[...] + lam[pl.ds(h * GZ + me, 1), :]
            rp = 1.0 / (1.0 + 0.5 * g + jnp.sqrt(g + 0.25 * g * g))
            for _ in range(XR.bit_length() - 1):
                rp = rp * rp
            full = rp
            for _ in range(XY.bit_length() - 1):
                full = full * full
            close = 1.0 / (1.0 - full)

            def piece(o, part):
                at = (h * XY + lax.rem(xi + o, XY)) * 2 * PR + part * PR
                return ag_v[pl.ds(pl.multiple_of(at, PR), PR), :]

            un, vn = piece(0, 0), piece(0, 1)
            for o in range(1, XY):
                un = un * rp + piece(o, 0)
                vn = vn * rp + piece(XY - o, 1)
            un = un * close
            vn = vn * close

            for i in range(NZ // BW):
                rows = pl.ds(h * NZ + i * BW, BW)
                at = home == -(i * QS)
                ub = jnp.where(at, jnp.concatenate([un] * QS, 0), 0.0)
                vb = jnp.where(at, jnp.concatenate([vn] * QS, 0), 0.0)
                step = 1
                while step < XL:
                    ub = ub + roll(ub, step * KL)
                    vb = vb + roll(vb, step * KL)
                    step *= 2
                ea_v[rows, :] = ea_v[rows, :] + up_v[rows, :] * ub
                eb_v[rows, :] = eb_v[rows, :] + dn_v[rows, :] * vb

            def finish(i, _):
                rows = pl.ds(pl.multiple_of(h * NZ + i * BR, BR), BR)
                out = pl.ds(pl.multiple_of(i * BR, BR), BR)
                r = r_v[rows, :]
                c = c_v[rows, :]
                cu = [r * ea_v[rows, :]]
                cv = [r * eb_v[rows, :]]
                for _ in range(J - 1):
                    cu.append(r * cu[-1])
                    cv.append(r * cv[-1])
                for j in range(J):
                    col = pl.ds(j * 128, 128)
                    a, b = split(c * (x_v[rows, col] + cu[j] + cv[J - 1 - j]))
                    dh[out, col] = a
                    dl[out, col] = b
                return 0

            lax.fori_loop(0, NZ // BR, finish, 0)

        with jax.named_scope("idst"):
            for c in range(W // 256):
                col = pl.ds(c * 256, 256)
                send2[pl.ds(h * NZ, NZ), col] = dot3((sh[...], sl[...]), (dh[:, col], dl[:, col]))

        with jax.named_scope("back"):
            mine = tile8(h * GZ + spot)

            for o in far_first():
                to = peer(o)
                remote(send2.at[tile8(h * GZ + to)], recv2.at[mine], b_s.at[h], b_r.at[h], {"gz": to})
            recv2[mine, :] = send2[tile8(h * GZ + me), :]

    for k in range(NH + LAG):
        if k < NH:
            descend(k)
        if k >= LAG:
            ascend(k - LAG)

    def neighbours():
        total = None
        for h in range(NH):
            for c in planes[h]:
                c.wait()
            rows, hrow = pl.ds(h * EDGE, EDGE), pl.ds(h * LH, LH)
            part = dot3(split(zb_v[rows, :] - zq_v[rows, :]), (hh[hrow, :], hl[hrow, :]))
            total = part if h == 0 else total + part
        ph_v[...] = total

    planes = []
    for h in range(NH):
        hrow = pl.ds(h * LH, LH)
        with jax.named_scope("waitback"):
            wait_bytes(recv2.at[pl.ds(h * NZ, NZ - 8)], b_r.at[h])

        with jax.named_scope("unpack"):
            for t in range(NG):
                for j in range(J):
                    tiles = exchange_lanes(
                        [recv2[pl.ds((h * GZ + t * XL + a) * 8, 8), pl.ds(j * 128, 128)] for a in range(XL)]
                    )
                    for a in range(XL):
                        zz_v[pl.ds((a * J + j) * 8, 8), pl.ds(t * 128, 128)] = tiles[a]

        with jax.named_scope("planes"):
            edge0 = h * EDGE

            def border(i, _):
                for k in range(8):
                    x = i * 8 + k
                    zb_v[pl.ds(edge0 + x, 1), :] = zz_v[pl.ds(x * 8, 1), :]
                    zb_v[pl.ds(edge0 + XR + x, 1), :] = zz_v[pl.ds(x * 8 + 7, 1), :]
                return 0

            lax.fori_loop(0, XR // 8, border, 0)
            zb_v[pl.ds(edge0 + 2 * XR, 8), :] = zz_v[pl.ds(0, 8), :]
            zb_v[pl.ds(edge0 + 2 * XR + 8, 8), :] = zz_v[pl.ds(ROWS - 8, 8), :]
            routes = (
                (XR, 0, XR, True),
                (0, XR, XR, False),
                (2 * XR + 8, 2 * XR, 8, xy(1)),
                (2 * XR, 2 * XR + 8, 8, xy(XY - 1)),
            )
            planes.append([
                (Shift if k < 2 else remote)(
                    zb_v.at[pl.ds(edge0 + a, size)], zq_v.at[pl.ds(edge0 + b, size)],
                    ph_s.at[4 * h + k], ph_r.at[4 * h + k], who,
                )
                for k, (a, b, size, who) in enumerate(routes)
            ])

        with jax.named_scope("inverse"):
            def inverse(i, _):
                rows = pl.ds(pl.multiple_of(i * 256, 256), 256)
                out = rows
                part = dot3(split(zz_v[rows, :]), (hh[hrow, :], hl[hrow, :]))
                p_v[out, :] = part if h == 0 else p_v[out, :] + part
                return 0

            lax.fori_loop(0, ROWS // 256, inverse, 0)

    with jax.named_scope("outputs"):

        def outputs(i, _):
            def east(x, p, before):
                return f_v[tile8(x + 1), :] * f_v[tile8(x), :] * (e_v[tile8(x), :] - (p - before))

            p = p_v[tile8(i * 8), :]
            now = east(i * 8, p, p_v[tile8(jnp.maximum(i * 8 - 1, 0)), :])
            for k in range(8):
                x = i * 8 + k
                after = p_v[tile8(jnp.minimum(x + 1, XR - 1) if k == 7 else x + 1), :]
                then = east(x + 1, after, p)
                f = f_v[tile8(x + 1), :]
                north = f * pltpu.roll(f, 1, 1) * (n_v[tile8(x), :] - (p - pltpu.roll(p, 1, 1)))
                up = f * pltpu.roll(f, 1, 0) * (w_v[tile8(x), :] - (p - pltpu.roll(p, 1, 0)))
                up = jnp.where(sub == 0, 0.0, up)
                eo_v[tile8(x), :] = now
                no_v[tile8(x), :] = north
                wo_v[tile8(x), :] = up
                ro_v[tile8(x), :] = (now - then) + (north - pltpu.roll(north, NY - 1, 1)) + (up - pltpu.roll(up, 7, 0))
                now, p = then, after
            return 0

        lax.fori_loop(0, XR // 8, outputs, 0)

    with jax.named_scope("waitend"):
        for h in range(NH):
            wait_bytes(send1.at[pl.ds(h * NZ, NZ - 8)], a_s.at[h])
            wait_bytes(ag_v.at[pl.ds(h * XY * 2 * PR, (XY - 1) * 2 * PR)], g_s.at[h])
            wait_bytes(send2.at[pl.ds(h * NZ, NZ - 8)], b_s.at[h])
        halos[4].wait()
        neighbours()
    with jax.named_scope("faces"):
        west = f_v[pl.ds(8, 8), :] * fx_v[pl.ds(0, 8), :]
        west = west * (e_v[pl.ds(0, 8), :] - ph_v[pl.ds(2 * XR, 8), :])
        east = f_v[pl.ds(ROWS, 8), :] * fx_v[pl.ds(8, 8), :]
        east = east * (ex_v[...] + ph_v[pl.ds(2 * XR + 8, 8), :])
        eo_v[pl.ds(0, 8), :] = west
        ro_v[pl.ds(0, 8), :] = ro_v[pl.ds(0, 8), :] + west
        ro_v[pl.ds(ROWS - 8, 8), :] = ro_v[pl.ds(ROWS - 8, 8), :] - east
        z0_v[...] = zf_v[low, :] * (gs_v[...] - zs_v[high, :] * ph_v[low, :])
        z7_v[...] = zs_v[low, :] * (ga_v[...] + zf_v[high, :] * ph_v[high, :])


def last_kernel(p, e, n, w, r, z0, z7, eo, no, wo, po, ro, w_v, r_v, sem):
    copies = []

    def out(src, dst, part):
        rows = pl.ds(part * XS * 8, XS * 8)
        copies.append(pltpu.make_async_copy(src.at[rows], dst.at[rows], sem.at[len(copies)]))
        copies[-1].start()

    for src, dst in ((e, eo), (n, no), (p, po)):
        for part in range(XR // XS):
            out(src, dst, part)
    sub = lax.broadcasted_iota(jnp.int32, (8, NY), 0)
    for s in range(XR // XS):

        def one(i, _):
            for k in range(8):
                x = s * XS + i * 8 + k
                face = row(z0, x)
                w_v[tile8(x), :] = jnp.where(sub == 0, face, w[tile8(x), :])
                r_v[tile8(x), :] = r[tile8(x), :] + jnp.where(sub == 0, face, jnp.where(sub == 7, -row(z7, x), 0.0))
            return 0

        lax.fori_loop(0, XS // 8, one, 0)
        out(w_v, wo, s)
        out(r_v, ro, s)
    for c in copies:
        c.wait()


def tables():
    i = np.arange(NY)
    angle = 2 * np.pi * ((i[:, None] * i[None, :]) % NY) / NY
    hart = np.cos(angle) + np.sin(angle)
    k = np.arange(1, NZ + 1)
    sine = np.sin(np.pi * ((k[:, None] * k[None, :]) % (2 * (NZ + 1))) / (NZ + 1))
    lam = 4 * np.sin(np.pi * i / NY) ** 2
    mu = 4 * np.sin(np.pi * k / (2 * (NZ + 1))) ** 2

    def cut(a):
        hi = a.astype(np.float32).astype(BF16)
        return hi, (a - hi.astype(np.float64)).astype(np.float32).astype(BF16)

    lanes_of = np.arange(128)
    half = np.arange(NH)[:, None, None]
    who = slot(np.arange(GZ))[None, :, None]
    lam = lam[half * LH + who * KL + lanes_of[None, None, :] % KL].reshape(NH * GZ, 128)
    packed = mu[(lanes_of[None, :] // KL) * PR + np.arange(PR)[:, None]]
    mu = np.repeat(mu[:, None], 128, 1)
    return (*cut(hart), *cut(sine), lam.astype(np.float32), mu.astype(np.float32), packed.astype(np.float32))


def local(east_velocity, north_velocity, upward_velocity, obstacle):
    fields = (east_velocity, north_velocity, upward_velocity, obstacle)
    args = [pltpu.with_memory_space_constraint(a.reshape(ROWS, NY), pltpu.HBM) for a in fields]
    args += [pltpu.with_memory_space_constraint(jnp.asarray(t), pltpu.HBM) for t in tables()]
    any_spec = pl.BlockSpec(memory_space=pl.ANY)
    vmem = pl.BlockSpec(memory_space=pltpu.VMEM)

    def v(*shape, dtype=F32):
        return pltpu.VMEM(shape, dtype)

    dma = pltpu.SemaphoreType.DMA
    field = jax.ShapeDtypeStruct((ROWS, NY), F32)
    plane = jax.ShapeDtypeStruct((XR, NY), F32)
    operands = pl.pallas_call(
        main_kernel,
        out_shape=[field] * 5 + [plane] * 2,
        in_specs=[any_spec] * 11,
        out_specs=[vmem] * 7,
        scratch_shapes=[
            v(ROWS + 16, NY), v(ROWS + 8, NY), v(ROWS, NY), v(ROWS, NY), v(2 * XR, NY), v(XR, NY),
            v(ROWS, NY, dtype=jnp.int32), v(ROWS, NY, dtype=BF16), v(ROWS, NY, dtype=BF16),
            v(NY, NY, dtype=BF16), v(NY, NY, dtype=BF16), v(NZ, NZ, dtype=BF16), v(NZ, NZ, dtype=BF16),
            v(NH * GZ, 128), v(NZ, 128), v(PR, 128),
            v(2 * XR, NY), v(XR, NY), v(16, NY), v(8, NY), v(EDGE, NY), v(EDGE, NY, dtype=BF16), v(EDGE, NY, dtype=BF16), v(EDGE, LH), v(NH * EDGE, LH), v(NH * EDGE, LH), v(EDGE, NY),
            v(NH * NZ, 128), v(NH * NZ, 128),
            v(NH * ROWS, LH), v(NH * NZ, W), v(NH * NZ, W), v(NZ, W, dtype=BF16), v(NZ, W, dtype=BF16),
            v(NH * NZ, W), v(NH * NZ, 128), v(NH * NZ, 128), v(NH * NZ, 128), v(NH * NZ, 128),
            v(NH * XY * 2 * PR, 128), v(NH * NZ, W), v(NH * NZ, W), v(ROWS, LH),
            dma((11,)), dma((6,)), dma((6,)), dma((NH,)), dma((NH,)), dma((NH,)), dma((NH,)),
            dma((NH,)), dma((NH,)), dma((4 * NH,)), dma((4 * NH,)),
        ],
        compiler_params=pltpu.CompilerParams(
            collective_id=0, has_side_effects=True, vmem_limit_bytes=32 * 1024 * 1024
        ),
        name="main",
    )(*args)

    outs = pl.pallas_call(
        last_kernel,
        out_shape=[field] * 5,
        in_specs=[vmem] * 7,
        out_specs=[any_spec] * 5,
        scratch_shapes=[v(ROWS, NY), v(ROWS, NY), dma((5 * (XR // XS),))],
        compiler_params=pltpu.CompilerParams(vmem_limit_bytes=8 * 1024 * 1024),
        name="last",
    )(*operands)
    return tuple(a.reshape(XR, CZ, NY) for a in outs)


def solution(mesh):
    spec = P("xy", "gz", None)
    return jax.shard_map(local, mesh=mesh, in_specs=(spec,) * 4, out_specs=(spec,) * 5, check_vma=False)
```
